32 devices in a mesh: dp: 16 (over z, y, x), tensor: 2 (over core).
Axes of the slice: x: 2, y: 2, z: 4, core: 2. Of those that a mesh axis runs over, the one named last changes fastest.
Arguments:
- residual: bfloat16 [512, 6144], P('dp', 'tensor'), may hold values from -16 to 16
- queries: bfloat16 [512, 6144], P('dp', 'tensor'), may hold values from -4.5 to 4.5
- keys: bfloat16 [512, 128, 1024], P('dp', None, 'tensor'), may hold values from -4.5 to 4.5
- values: bfloat16 [512, 128, 1024], P('dp', None, 'tensor'), may hold values from -6 to 6
- lengths: int32 [512], P('dp'), may hold values from 2 to 128
- norm_gain: bfloat16 [6144], P('tensor'), may hold values from 0.099609375 to 1.8984375
- expert_ids: int32 [512, 2], P('dp'), may hold values from 0 to 7, all different within a row; in each aligned block of 32 rows (0 to 31, 32 to 63, ...) at most 16 rows name the same one
- expert_weights: float32 [512, 2], P('dp'), may hold values from 0.2 to 1
- w_in: bfloat16 [6144, 65536], P('tensor', 'dp'), may hold values from -0.078125 to 0.078125
- w_out: bfloat16 [65536, 6144], P('dp', 'tensor'), may hold values from -0.0625 to 0.0625
Outputs:
- output: bfloat16 [512, 6144], P('dp', 'tensor')
The draws below stay inside these ranges and needn't reach their ends.
Inputs may be any that keep to these rules, and one draw needn't show every extreme that they name: `expert_ids`: each token names 2 different experts; at most 16 of the tokens of one index of dp name one expert, and in every draw some expert is named by exactly 16 of them.
All inputs are finite; a program needn't handle non-finite values.
Results may differ from the reference program's by a relative error of at most 0.008.
Values may be sent and summed in bfloat16 or wider, within the bound.
A program may use at most 128 MiB of HBM per device.

```python
import math
import jax
import jax.numpy as jnp
import numpy as np
from jax import lax

D = 6144
HEADS = 48
KV = 8
HEAD = 128
EXPERTS = 8
TOPK = 2
FF = 8192
CACHE = 128
TOK_DEV = 32
SRC_CAP = 16
TOKENS = 512
CAP = 96


def draw_residual(key, part):
    key_base, key_rough = jax.random.split(jax.random.fold_in(key, 101), 2)
    base = jax.random.normal(key_base, (TOKENS, D), jnp.float32)
    rough = jax.random.uniform(key_rough, (D,), jnp.float32, 0.5, 1.5)
    column = jnp.arange(D, dtype=jnp.float32) / (D - 1)
    rising = jnp.exp(math.log(3.0) * column) * 0.6
    drawn = base * rising[None, :] * rough[None, :]
    return jnp.clip(drawn, -16.0, 16.0).astype(jnp.bfloat16)


def attention_draw(key):
    key_query, key_cached = jax.random.split(jax.random.fold_in(key, 202), 2)
    queries = jnp.clip(jax.random.normal(key_query, (TOKENS, HEADS * HEAD), jnp.float32), -4.5, 4.5)
    cached = jnp.clip(jax.random.normal(key_cached, (TOKENS, CACHE, KV * HEAD), jnp.float32), -4.5, 4.5)
    return (queries.astype(jnp.bfloat16), cached.astype(jnp.bfloat16))


def draw_queries(key, part):
    return attention_draw(key)[0]


def draw_keys(key, part):
    return attention_draw(key)[1]


def touch_ends(values, key, smallest, top_value):
    longest = values.shape.index(max(values.shape))
    spots = []
    for shift in (0, 1):
        where = [jax.random.randint(jax.random.fold_in(key, axis), (), 0, length) for axis, length in enumerate(values.shape)]
        where[longest] = (where[longest] + shift) % values.shape[longest]
        spots.append(tuple(where))
    return values.at[spots[0]].set(smallest).at[spots[1]].set(top_value)


def steps_of(stream_key, dims, pieces, smallest, high):
    level, own = 1.0, jax.random.fold_in(stream_key, 6)
    for position, parts in pieces:
        draws = jnp.exp(jax.random.uniform(jax.random.fold_in(own, position), (parts,), jnp.float32, smallest / len(pieces), high / len(pieces)))
        level = level * jnp.repeat(draws, dims[position] // parts).reshape([-1 if axis == position else 1 for axis in range(len(dims))])
    return level


def assign_block(stream_key, own, number, rows, number_of, top, limit, lean):
    ranking = jax.random.permutation(stream_key, number_of)
    packed, usual = portions_of(number_of, rows * top, limit, lean, True), portions_of(number_of, rows * top, limit, lean, False)
    places = jnp.arange(number_of)

    def named(sizes, rotation):
        used = int((sizes > 0).sum())
        fixed = max(1, used // 4)
        passed = fixed + (places - fixed + rotation * (used - fixed)) % max(1, number_of - fixed)
        return jnp.zeros((number_of,), jnp.int32).at[ranking[jnp.where(places < fixed, places, passed)]].set(jnp.asarray(sizes, jnp.int32))

    sizes = jnp.where(number % 4 == 0, named(packed, number // 4), named(usual, number - number // 4 - 1))
    mixed = jax.random.permutation(jax.random.fold_in(own, 3), number_of)
    donor, sink = mixed[0:number_of // 2 * 2:2], mixed[1:number_of // 2 * 2:2]
    margin = jnp.minimum(sizes[donor] - 1, limit - sizes[sink]) // 2
    margin = jnp.where((donor == ranking[0]) | (sink == ranking[0]) | (sizes[sink] == 0), 0, jnp.maximum(margin, 0))
    passed = jax.random.randint(jax.random.fold_in(own, 4), (number_of // 2,), 0, 1 << 20) % (margin + 1)
    sizes = sizes.at[donor].add(-passed).at[sink].add(passed)
    items = jnp.searchsorted(jnp.cumsum(sizes), jnp.arange(rows * top), side="right").astype(jnp.int32)
    table = items.reshape(top, rows).T
    table = table[jax.random.permutation(jax.random.fold_in(own, 1), rows)]
    rotation = jax.random.randint(jax.random.fold_in(own, 2), (rows, 1), 0, top)
    return jnp.take_along_axis(table, (jnp.arange(top)[None, :] + rotation) % top, axis=1)


def portions_of(amount, total, reach, lean, full):
    portions = [(1 << 20) // math.isqrt(standing ** lean) + 1 for standing in range(1, amount + 1)]
    largest = reach if full else min(reach, max(-(-total // amount), total * portions[0] // sum(portions)))
    least = 1 if total - largest >= amount - 1 else 0
    holding, rest = [largest] + [least] * (amount - 1), total - largest - least * (amount - 1)
    while rest > 0:
        movable = [i for i in range(1, amount) if holding[i] < largest] or [i for i in range(1, amount) if holding[i] < reach]
        mass, budget = sum([portions[i] for i in movable]), rest
        for i in movable:
            more = min(reach - holding[i], max(1, budget * portions[i] // mass), rest)
            holding[i] = holding[i] + more
            rest = rest - more
    return np.array(holding)


def normal_values(key, shape, width, most, cuts=(), kind=jnp.bfloat16):
    values = width * jax.random.normal(key, shape, jnp.float32)
    if cuts:
        values = values * steps_of(key, shape, cuts, -0.22, 0.18)
    return jnp.clip(values, -most, most).astype(kind)


def setup_inputs(seed: int = 0) -> dict:
    streams_of = jax.random.split(jax.random.key(seed), 11)
    residual = draw_residual(jax.random.fold_in(streams_of[10], 71), 0)
    queries = draw_queries(jax.random.fold_in(streams_of[10], 71), 0)
    keys = draw_keys(jax.random.fold_in(streams_of[10], 71), 0)
    values = normal_values(streams_of[3], (TOKENS, CACHE, KV * HEAD), 1.0, 6.0, ((0, 16), (2, 2)))
    lengths = touch_ends(jax.random.randint(streams_of[4], (TOKENS,), 2, CACHE + 1), jax.random.fold_in(streams_of[4], 1), 2, CACHE).astype(jnp.int32)
    norm_gain = jnp.clip(1.0 + 0.18 * jax.random.normal(streams_of[5], (D,), jnp.float32), 0.099609375, 1.8984375).astype(jnp.bfloat16)
    expert_ids_keys = jax.random.split(jax.random.fold_in(streams_of[6], 1), TOKENS // TOK_DEV)
    expert_ids_turns = jax.random.permutation(jax.random.fold_in(streams_of[6], 3), TOKENS // TOK_DEV)
    expert_ids = jax.vmap(lambda own, number: assign_block(jax.random.fold_in(streams_of[6], 2), own, number, TOK_DEV, EXPERTS, TOPK, SRC_CAP, 2))(expert_ids_keys, expert_ids_turns).reshape((TOKENS, TOPK))
    expert_weights = jnp.clip(0.2 + 0.8 * jax.random.uniform(streams_of[7], (TOKENS, TOPK), jnp.float32) ** steps_of(streams_of[7], (TOKENS, TOPK), ((0, 16),), -0.2, 0.2), 0.2, 1.0)
    w_in = normal_values(streams_of[8], (D, EXPERTS * FF), D ** -0.5, 0.078125, ((0, 2), (1, 16)))
    w_out = normal_values(streams_of[9], (EXPERTS * FF, D), FF ** -0.5, 0.0625, ((0, 16), (1, 2)))
    return {"residual": residual, "queries": queries, "keys": keys, "values": values, "lengths": lengths, "norm_gain": norm_gain, "expert_ids": expert_ids, "expert_weights": expert_weights, "w_in": w_in, "w_out": w_out}


NORM_EPSILON = 1e-05

def attention_rows(residual, queries, keys, values, lengths):
    group_size = HEADS // KV
    query_float = queries.astype(jnp.float32).reshape(TOKENS, KV, group_size, HEAD)
    key_float = keys.astype(jnp.float32).reshape(TOKENS, CACHE, KV, HEAD)
    value_float = values.astype(jnp.float32).reshape(TOKENS, CACHE, KV, HEAD)
    scores = jnp.einsum('tgjd,tlgd->tgjl', query_float, key_float) * HEAD ** (-0.5)
    live_mask = (jnp.arange(CACHE, dtype=jnp.int32)[None, :] < lengths[:, None])[:, None, None, :]
    scores = jnp.where(live_mask, scores, -1e+30)
    peak_score = lax.optimization_barrier(jnp.max(scores, axis=-1, keepdims=True))
    powered = jnp.exp(scores - peak_score)
    attention_probs = (powered / lax.optimization_barrier(jnp.sum(powered, axis=-1, keepdims=True))).astype(jnp.bfloat16)
    attended = jnp.einsum('tgjl,tlgd->tgjd', attention_probs.astype(jnp.float32), value_float)
    return residual.astype(jnp.float32) + attended.reshape(TOKENS, D)

def reference(residual, queries, keys, values, lengths, norm_gain, expert_ids, expert_weights, w_in, w_out):
    summed = attention_rows(residual, queries, keys, values, lengths)
    square_sums = lax.optimization_barrier(jnp.sum(summed * summed, axis=1, keepdims=True))
    normed = (summed * lax.rsqrt(square_sums / D + NORM_EPSILON) * norm_gain.astype(jnp.float32)).astype(jnp.bfloat16)
    flat_ids = expert_ids.reshape(-1)
    pair_count = TOKENS * TOPK
    onehot = (flat_ids[:, None] == jnp.arange(EXPERTS, dtype=jnp.int32)[None, :]).astype(jnp.int32)
    earlier = jnp.cumsum(onehot, axis=0, dtype=jnp.int32) - onehot
    slot_index = lax.optimization_barrier(jnp.sum(earlier * onehot, axis=1, dtype=jnp.int32))
    capacity = CAP
    keep_mask = slot_index < capacity
    token_index = jnp.arange(pair_count, dtype=jnp.int32) // TOPK
    padded_rows = jnp.concatenate([normed, jnp.zeros((1, D), jnp.bfloat16)], axis=0)
    pair_out = jnp.zeros((pair_count, D), jnp.float32)
    for expert in range(EXPERTS):
        chosen = (flat_ids == expert) & keep_mask
        target = jnp.where(chosen, slot_index, capacity).astype(jnp.int32)
        source_row = jnp.full((capacity,), TOKENS, jnp.int32).at[target].set(token_index, mode='drop')
        gathered = padded_rows[source_row]
        hidden = jax.nn.silu(jnp.dot(gathered, w_in[:, expert * FF:(expert + 1) * FF], preferred_element_type=jnp.float32)).astype(jnp.bfloat16)
        produced = jnp.dot(hidden, w_out[expert * FF:(expert + 1) * FF], preferred_element_type=jnp.float32)
        padded_out = jnp.concatenate([produced, jnp.zeros((1, D), jnp.float32)], axis=0)
        pair_out = pair_out + padded_out[target]
    weighted = pair_out * expert_weights.reshape(-1)[:, None]
    output = summed + lax.optimization_barrier(jnp.sum(weighted.reshape(TOKENS, TOPK, D), axis=1))
    return output.astype(jnp.bfloat16)
```

```python
import functools

import jax
import jax.numpy as jnp
from jax import lax
from jax.experimental import pallas as pl
from jax.experimental.pallas import tpu as pltpu
from jax.sharding import PartitionSpec as P

D = 6144
HEADS = 48
KV = 8
HEAD = 128
EXPERTS = 8
TOPK = 2
CACHE = 128
SRC_CAP = 16


NORM_EPSILON = 1e-05


MESH = pl.DeviceIdType.MESH


def remote(source, target, send_sem, recv_sem, place):
    return pltpu.make_async_remote_copy(
        src_ref=source,
        dst_ref=target,
        send_sem=send_sem,
        recv_sem=recv_sem,
        device_id={"dp": place},
        device_id_type=MESH,
    )


def greet(places):
    barrier = pltpu.get_barrier_semaphore()
    for place in places:
        pl.semaphore_signal(barrier, inc=1, device_id={"dp": place}, device_id_type=MESH)
    pl.semaphore_wait(barrier, len(places))


def far_first(amount):
    return sorted(range(1, amount), key=lambda lap: (-min(lap, amount - lap), lap))


def dispatch_kernel(owners, packed, counts, received, all_counts, plane_send, plane_recv,
                    pair_send, pair_recv, count_send, count_recv, own_sem):
    experts = packed.shape[0]
    places = experts * owners
    me = lax.axis_index("dp")
    expert, owner = lax.div(me, owners), lax.rem(me, owners)
    greet([lax.rem(me + lap, places) for lap in range(1, places)])
    waiting = []
    for lap in range(1, places):
        copy = remote(counts, all_counts.at[me], count_send.at[lap], count_recv.at[lap],
                      lax.rem(me + lap, places))
        copy.start()
        waiting.append(copy)
    own = pltpu.make_async_copy(packed.at[expert], received.at[me], own_sem)
    own.start()
    own_count = pltpu.make_async_copy(counts, all_counts.at[me], count_recv.at[0])
    own_count.start()

    def forward(source, place, lap):
        for step in range(1, owners):
            other = lax.rem(owner + step, owners)
            spot = lap * owners + step
            copy = remote(source, received.at[place], pair_send.at[spot], pair_recv.at[spot],
                          expert * owners + other)
            copy.start()
            waiting.append(copy)

    forward(packed.at[expert], me, 0)
    middle = far_first(experts)
    order = [lap for lap in middle if lap in (1, experts - 1)]
    order += [lap for lap in middle if lap not in (1, experts - 1)]
    for lap in order:
        target = lax.rem(expert + lap, experts)
        copy = remote(packed.at[target], received.at[me], plane_send.at[lap], plane_recv.at[lap],
                      target * owners + owner)
        copy.start()
        waiting.append(copy)
    for lap in order:
        source = lax.rem(expert + experts - lap, experts) * owners + owner
        remote(received.at[source], received.at[source], plane_send.at[lap], plane_recv.at[lap],
               source).wait_recv()
        forward(received.at[source], source, lap)
    for lap in [0] + order:
        for step in range(1, owners):
            other = lax.rem(owner + owners - step, owners)
            place = lax.rem(expert + experts - lap, experts) * owners + other
            spot = lap * owners + step
            remote(received.at[place], received.at[place], pair_send.at[spot], pair_recv.at[spot],
                   expert * owners + other).wait_recv()
    for lap in range(1, places):
        source = lax.rem(me + places - lap, places)
        remote(counts, all_counts.at[source], count_send.at[lap], count_recv.at[lap],
               source).wait_recv()
    own.wait()
    own_count.wait()
    for copy in waiting:
        copy.wait_send()


def dispatch(packed, counts, owners):
    experts, rows, width = packed.shape
    places = experts * owners
    dma = pltpu.SemaphoreType.DMA
    vmem = pl.BlockSpec(memory_space=pltpu.VMEM)
    return pl.pallas_call(
        functools.partial(dispatch_kernel, owners),
        out_shape=(
            jax.ShapeDtypeStruct((places, rows, width), packed.dtype),
            jax.ShapeDtypeStruct((places,) + counts.shape, counts.dtype),
        ),
        in_specs=[vmem, vmem],
        out_specs=(vmem, vmem),
        scratch_shapes=[
            dma((experts,)),
            dma((experts,)),
            dma((places,)),
            dma((places,)),
            dma((places,)),
            dma((places,)),
            dma,
        ],
        compiler_params=pltpu.CompilerParams(collective_id=0, has_side_effects=True),
    )(packed, counts)


def return_kernel(owners, part, out, landed, total, pair_send, pair_recv, plane_send, plane_recv):
    experts = out.shape[0]
    me = lax.axis_index("dp")
    expert, owner = lax.div(me, owners), lax.rem(me, owners)
    greet(
        [lax.rem(expert + lap, experts) * owners + owner for lap in range(1, experts)]
        + [expert * owners + lax.rem(owner + step, owners) for step in range(1, owners)]
    )
    order = far_first(experts) + [0]
    waiting = []
    for lap in order:
        for step in range(1, owners):
            other = lax.rem(owner + step, owners)
            source = lax.rem(expert + lap, experts) * owners + other
            spot = lap * owners + step
            copy = remote(part.at[source], landed.at[spot], pair_send.at[spot], pair_recv.at[spot],
                          expert * owners + other)
            copy.start()
            waiting.append(copy)
    for lap in order:
        target = lax.rem(expert + lap, experts) * owners + owner
        value = part[target].astype(jnp.float32)
        for step in range(1, owners):
            other = lax.rem(owner + owners - step, owners)
            spot = lap * owners + step
            remote(landed.at[spot], landed.at[spot], pair_send.at[spot], pair_recv.at[spot],
                   expert * owners + other).wait_recv()
            value += landed[spot].astype(jnp.float32)
        if lap == 0:
            out[expert] = value.astype(out.dtype)
        else:
            total[lap] = value.astype(total.dtype)
            copy = remote(total.at[lap], out.at[expert], plane_send.at[lap], plane_recv.at[lap],
                          target)
            copy.start()
            waiting.append(copy)
    for lap in order[:-1]:
        source = lax.rem(expert + experts - lap, experts)
        remote(total.at[lap], out.at[source], plane_send.at[lap], plane_recv.at[lap],
               source * owners + owner).wait_recv()
    for copy in waiting:
        copy.wait_send()


def send_back(part, owners):
    places, rows, width = part.shape
    experts = places // owners
    dma = pltpu.SemaphoreType.DMA
    vmem = pl.BlockSpec(memory_space=pltpu.VMEM)
    return pl.pallas_call(
        functools.partial(return_kernel, owners),
        out_shape=jax.ShapeDtypeStruct((experts, rows, width), part.dtype),
        in_specs=[vmem],
        out_specs=vmem,
        scratch_shapes=[
            pltpu.VMEM((places, rows, width), part.dtype),
            pltpu.VMEM((experts, rows, width), part.dtype),
            dma((places,)),
            dma((places,)),
            dma((experts,)),
            dma((experts,)),
        ],
        compiler_params=pltpu.CompilerParams(collective_id=1, has_side_effects=True),
    )(part)


def hidden_kernel(members, chunk, part, out, landed, send_sem, recv_sem):
    me = lax.axis_index("tensor")
    barrier = pltpu.get_barrier_semaphore()
    for step in range(1, members):
        pl.semaphore_signal(
            barrier,
            inc=1,
            device_id={"tensor": lax.rem(me + step, members)},
            device_id_type=MESH,
        )
    pl.semaphore_wait(barrier, members - 1)

    def piece_copy(piece, step):
        rows = pl.ds(piece * chunk, chunk)
        spot = piece * members + step
        return pltpu.make_async_remote_copy(
            src_ref=part.at[rows],
            dst_ref=landed.at[step, rows],
            send_sem=send_sem.at[spot],
            recv_sem=recv_sem.at[spot],
            device_id={"tensor": lax.rem(me + step, members)},
            device_id_type=MESH,
        )

    copies = [
        [piece_copy(piece, step) for step in range(1, members)]
        for piece in range(part.shape[0] // chunk)
    ]
    for row in copies:
        for copy in row:
            copy.start()
    for piece, row in enumerate(copies):
        rows = pl.ds(piece * chunk, chunk)
        value = part[rows].astype(jnp.float32)
        for step, copy in enumerate(row, 1):
            copy.wait_recv()
            value += landed[step, rows].astype(jnp.float32)
        out[rows] = (value / (1.0 + jnp.exp(-value))).astype(out.dtype)
    for row in copies:
        for copy in row:
            copy.wait_send()


def hidden_rows(part):
    members = lax.axis_size("tensor")
    rows = part.shape[0]
    chunk = 32 if rows % 32 == 0 else rows
    dma = pltpu.SemaphoreType.DMA
    vmem = pl.BlockSpec(memory_space=pltpu.VMEM)
    return pl.pallas_call(
        functools.partial(hidden_kernel, members, chunk),
        out_shape=jax.ShapeDtypeStruct(part.shape, part.dtype),
        in_specs=[vmem],
        out_specs=vmem,
        scratch_shapes=[
            pltpu.VMEM((members,) + part.shape, part.dtype),
            dma((members * (rows // chunk),)),
            dma((members * (rows // chunk),)),
        ],
        compiler_params=pltpu.CompilerParams(collective_id=2, has_side_effects=True),
    )(part)


def expert_rows(tok_rows, w_in, w_out):
    partial_sum = jnp.einsum("rd,df->rf", tok_rows, w_in, preferred_element_type=jnp.float32)
    hidden = hidden_rows(partial_sum.astype(jnp.bfloat16))
    return jnp.einsum("rf,fd->rd", hidden, w_out, preferred_element_type=jnp.float32)


def slots_of(rows):
    return -(-rows // 128) * 128


def layer_kernel(dims, summed, gain, named, w_in, w_out, out, win, wout, squares, squares_in, gath,
                 nrm, tok, pick, pick_t, slot_weight, sendx, gotx, acc, part, part_in, hidden,
                 sendy, goty, weighted, line_out, line_in, fin, extra,
                 in_sem, out_sem, sq_sem, gath_sem, first_sem, line_sem, third_sem, part_sem,
                 back_sem, relay_sem, home_sem):
    lines, planes, owners, chunks, capacity = dims
    tokens, width = summed.shape
    members = planes * owners
    places = lines * members
    quarter = width // members
    cols = quarter // chunks
    group = members * tokens
    slots = slots_of(capacity)
    units = w_in.shape[1]
    me = lax.axis_index("dp")
    line, spot = lax.div(me, members), lax.rem(me, members)
    own_plane = lax.div(spot, owners)
    other_core = 1 - lax.axis_index("tensor")
    f32, bf16 = jnp.float32, jnp.bfloat16

    def far(source, target, sems, index, device):
        return pltpu.make_async_remote_copy(
            src_ref=source, dst_ref=target, send_sem=sems.at[(0,) + index],
            recv_sem=sems.at[(1,) + index], device_id=device, device_id_type=MESH,
        )

    def peer(step):
        return lax.rem(spot + step, members)

    def sender(step):
        return lax.rem(spot + members - step, members)

    def place(index):
        return {"dp": line * members + index}

    steps = range(1, members)
    win_copies = [
        [
            pltpu.make_async_copy(
                w_in.at[pl.ds(q * quarter + c * cols, cols)],
                win.at[pl.ds((c * members + q) * cols, cols)],
                in_sem.at[c, q],
            )
            for q in range(members)
        ]
        for c in range(chunks)
    ]
    pieces = out_sem.shape[0]
    piece = units // pieces
    wout_copies = [
        pltpu.make_async_copy(
            w_out.at[pl.ds(i * piece, piece)], wout.at[pl.ds(i * piece, piece)], out_sem.at[i]
        )
        for i in range(pieces)
    ]
    barrier = pltpu.get_barrier_semaphore()
    for lap in range(1, places):
        pl.semaphore_signal(
            barrier, inc=1, device_id={"dp": lax.rem(me + lap, places)}, device_id_type=MESH
        )
    pl.semaphore_signal(barrier, inc=1, device_id={"tensor": other_core}, device_id_type=MESH)
    for row in win_copies:
        for copy in row:
            copy.start()
    for copy in wout_copies:
        copy.start()
    total = jnp.zeros((tokens, 1), f32)
    for q in range(members * chunks):
        value = summed[:, q * cols:(q + 1) * cols]
        total += jnp.sum(value * value, axis=1, keepdims=True)
    squares[...] = jnp.broadcast_to(total, squares.shape)
    pl.semaphore_wait(barrier, places)
    waiting = []
    square_copy = far(squares, squares_in, sq_sem, (), {"tensor": other_core})
    square_copy.start()
    waiting.append(square_copy)
    for lap in range(1, places):
        copy = far(named, gath.at[me], gath_sem, (lap,), {"dp": lax.rem(me + lap, places)})
        copy.start()
        waiting.append(copy)
    gath[me] = named[...]
    square_copy.wait_recv()
    scale = lax.rsqrt(
        (squares[:, :1] + squares_in[:, :1]) / (2 * width) + NORM_EPSILON
    )
    for c in range(chunks):
        for q in range(members):
            at = q * quarter + c * cols
            nrm[q, c] = (
                summed[:, at:at + cols] * scale * gain[:, at:at + cols].astype(f32)
            ).astype(bf16)
        home = pl.ds(pl.multiple_of(line * group + spot * tokens, tokens), tokens)
        tok[c, home] = nrm[spot, c]
        for step in steps:
            copy = far(nrm.at[peer(step), c], tok.at[c, home], first_sem, (c, step),
                       place(peer(step)))
            copy.start()
            waiting.append(copy)

    def rows_of(plane):
        return pl.ds(pl.multiple_of(plane * group, group), group)

    def inside(plane):
        return (plane >= 0) & (plane < lines)

    def spread(way, c, gap):
        turn = 1 - 2 * way
        plane = line - gap * turn
        rows = rows_of(plane)
        return inside(plane) & inside(line + turn), far(
            tok.at[c, rows], tok.at[c, rows], line_sem, (way, c, plane),
            {"dp": me + turn * members},
        )

    def arrive(way, c, gap):
        plane = line - gap * (1 - 2 * way)
        rows = rows_of(plane)
        return inside(plane), far(
            tok.at[c, rows], tok.at[c, rows], line_sem, (way, c, plane), {"dp": me}
        )

    def begin(pair):
        @pl.when(pair[0])
        def _():
            pair[1].start()

    def landed(pair):
        @pl.when(pair[0])
        def _():
            pair[1].wait_recv()

    def left(pair):
        @pl.when(pair[0])
        def _():
            pair[1].wait_send()

    for c in range(chunks):
        for step in steps:
            rows = pl.ds(pl.multiple_of(line * group + sender(step) * tokens, tokens), tokens)
            far(nrm.at[0, c], tok.at[c, rows], first_sem, (c, step),
                place(sender(step))).wait_recv()
        for way in (0, 1):
            begin(spread(way, c, 0))

    for lap in range(1, places):
        source = lax.rem(me + places - lap, places)
        far(named, gath.at[source], gath_sem, (lap,), {"dp": source}).wait_recv()
    hits, weights = [], []
    for p in range(lines):
        tile = gath[p * members]
        for m in range(1, members):
            tile += gath[p * members + m]
        for b in range(planes):
            expert = (line * planes + b).astype(f32)
            first, second = tile[0:1] == expert, tile[1:2] == expert
            hits.append(jnp.where(first | second, 1.0, 0.0))
            weights.append(jnp.where(first, tile[2:3], jnp.where(second, tile[3:4], 0.0)))
    earlier = lax.broadcasted_iota(jnp.int32, (group, group), 0)
    later = lax.broadcasted_iota(jnp.int32, (group, group), 1)
    before = jnp.where(earlier < later, 1.0, 0.0).astype(bf16)
    slot_iota = lax.broadcasted_iota(jnp.int32, (slots, group), 0).astype(f32)
    for b in range(planes):
        offset = jnp.zeros((1, 1), f32)
        slot_total = jnp.zeros((slots, 1), f32)
        for p in range(lines):
            hit, weight = hits[p * planes + b], weights[p * planes + b]
            wide = jnp.broadcast_to(hit, (16, group)).astype(bf16)
            rank = jnp.dot(wide, before, preferred_element_type=f32)[0:1] + offset
            offset += jnp.sum(hit, axis=1, keepdims=True)
            rank = jnp.where((hit > 0.0) & (rank < capacity), rank, -1.0)
            chosen = jnp.where(slot_iota == rank, 1.0, 0.0)
            pick[b * slots:(b + 1) * slots, p * group:(p + 1) * group] = chosen.astype(bf16)
            pick_t[p, :, b * slots:(b + 1) * slots] = chosen.T.astype(bf16)
            slot_total += jnp.sum(chosen * weight, axis=1, keepdims=True)
        slot_weight[b * slots:(b + 1) * slots] = jnp.broadcast_to(slot_total, (slots, 128))
    weighted[...] = jnp.zeros_like(weighted)

    def lanes_of(index):
        return pl.ds(pl.multiple_of(index * cols, 128), cols)

    depth = members * cols
    block = 512
    spans = part.shape[0]
    span = units // spans

    def product(c, at):
        at = pl.multiple_of(at, 128)
        return jnp.dot(gotx[c], win[c * depth:(c + 1) * depth, pl.ds(at, block)],
                       preferred_element_type=f32)

    def expand(c):
        for step in steps:
            far(sendx.at[c, 0], gotx.at[c, :, lanes_of(sender(step))], third_sem, (c, step),
                place(sender(step))).wait_recv()
        for copy in win_copies[c]:
            copy.wait()
        if c < chunks - 1:
            @pl.loop(0, units // block)
            def _(i):
                at = pl.multiple_of(i * block, block)
                value = product(c, at)
                acc[:, pl.ds(at, block)] = value if c == 0 else acc[:, pl.ds(at, block)] + value
            return
        for h in range(spans):
            @pl.loop(0, span // block)
            def _(i):
                inner = pl.multiple_of(i * block, block)
                at = h * span + inner
                value = product(c, at)
                if c:
                    value += acc[:, pl.ds(pl.multiple_of(at, block), block)]
                part[h, :, pl.ds(inner, block)] = value.astype(bf16)
            copy = far(part.at[h], part_in.at[h], part_sem, (h,), {"tensor": other_core})
            copy.start()
            waiting.append(copy)

    for c in range(chunks):
        for gap in range(1, lines):
            for way in (0, 1):
                landed(arrive(way, c, gap))
                begin(spread(way, c, gap))
        rows = jnp.dot(pick[...], tok[c], preferred_element_type=f32).astype(bf16)
        for b in range(planes):
            sendx[c, b] = rows[b * slots:b * slots + capacity]
        for step in steps:
            copy = far(sendx.at[c, lax.div(peer(step), owners)], gotx.at[c, :, lanes_of(spot)],
                       third_sem, (c, step), place(peer(step)))
            copy.start()
            waiting.append(copy)
        gotx[c, :, lanes_of(spot)] = sendx[c, own_plane]
        if c:
            expand(c - 1)
    expand(chunks - 1)
    for h in range(spans):
        far(part.at[h], part_in.at[h], part_sem, (h,), {"tensor": other_core}).wait_recv()

        @pl.loop(0, span // block)
        def _(i):
            at = pl.ds(pl.multiple_of(i * block, block), block)
            value = part[h, :, at].astype(f32) + part_in[h, :, at].astype(f32)
            value = value / (1.0 + jnp.exp(-value))
            hidden[:, pl.ds(pl.multiple_of(h * span + i * block, block), block)] = (
                value.astype(bf16)
            )
    for copy in wout_copies:
        copy.wait()

    def contract(c):
        for step in list(steps) + [0]:
            at = pl.multiple_of(peer(step) * quarter + c * cols, 128)
            value = jnp.dot(hidden[...], wout[:, pl.ds(at, cols)], preferred_element_type=f32)
            if step:
                sendy[c, step - 1] = value.astype(bf16)
                copy = far(sendy.at[c, step - 1], goty.at[c, spot], back_sem, (c, step),
                           place(peer(step)))
                copy.start()
                waiting.append(copy)
            else:
                goty[c, spot] = value.astype(bf16)

    def gather_back(c):
        for step in steps:
            far(sendy.at[c, 0], goty.at[c, sender(step)], back_sem, (c, step),
                place(sender(step))).wait_recv()
        for b in range(planes):
            value = goty[c, b * owners].astype(f32)
            for o in range(1, owners):
                value += goty[c, b * owners + o].astype(f32)
            value = value * slot_weight[b * slots:b * slots + capacity, :1]
            weighted[c, b * slots:b * slots + capacity] = value.astype(bf16)

    def share(c, plane):
        return jnp.dot(pick_t[plane], weighted[c], preferred_element_type=f32)

    def relay_copy(way, c, plane, place_index):
        return far(line_out.at[way, c, plane], line_in.at[way, c, plane], relay_sem,
                   (way, c, plane), {"dp": place_index})

    def relay(way, c, gap):
        turn = 1 - 2 * way
        plane = line + gap * turn

        @pl.when(inside(plane))
        def _():
            value = share(c, plane)
            line_out[way, c, plane] = value.astype(bf16)

            @pl.when(inside(line - turn))
            def _():
                relay_copy(way, c, plane, me - turn * members).wait_recv()
                line_out[way, c, plane] = (
                    value + line_in[way, c, plane].astype(f32)
                ).astype(bf16)

            relay_copy(way, c, plane, me + turn * members).start()

    near = jnp.where(line * 2 < lines, 0, 1)

    def home_copy(c, step):
        rows = pl.ds(pl.multiple_of(peer(step) * tokens, tokens), tokens)
        return far(fin.at[c, rows], extra.at[c, spot], home_sem, (c, step), place(peer(step)))

    def finish(c):
        fin[c] = share(c, line).astype(bf16)
        for way in (0, 1):
            turn = 1 - 2 * way

            @pl.when(inside(line - turn))
            def _():
                relay_copy(way, c, line, me - turn * members).wait_recv()

        low, high = line > 0, line < lines - 1

        def got(way):
            return line_in[way, c, line].astype(f32)

        @pl.when(low & high)
        def _():
            fin[c] = (share(c, line) + got(0) + got(1)).astype(bf16)

        @pl.when(low & ~high)
        def _():
            fin[c] = (share(c, line) + got(0)).astype(bf16)

        @pl.when(high & ~low)
        def _():
            fin[c] = (share(c, line) + got(1)).astype(bf16)

        for step in steps:
            copy = home_copy(c, step)
            copy.start()
            waiting.append(copy)
        extra[c, spot] = fin[c, pl.ds(pl.multiple_of(spot * tokens, tokens), tokens)]

    def close(c):
        for step in steps:
            far(fin.at[c, pl.ds(0, tokens)], extra.at[c, sender(step)], home_sem, (c, step),
                place(sender(step))).wait_recv()
        for q in range(members):
            at = q * quarter + c * cols
            out[:, at:at + cols] = (
                summed[:, at:at + cols] + extra[c, q].astype(f32)
            ).astype(out.dtype)

    for c in range(chunks):
        contract(c)
        if c:
            gather_back(c - 1)
            for gap in range(lines - 1, 1, -1):
                relay(near, c - 1, gap)
    gather_back(chunks - 1)
    for gap in range(lines - 1, 1, -1):
        relay(near, chunks - 1, gap)
    for c in range(chunks):
        relay(near, c, 1)
    for c in range(chunks):
        for gap in range(lines - 1, 0, -1):
            relay(1 - near, c, gap)
    for c in range(chunks):
        finish(c)
        if c:
            close(c - 1)
    close(chunks - 1)
    for copy in waiting:
        copy.wait_send()
    for c in range(chunks):
        for way in (0, 1):
            for gap in range(lines - 1):
                left(spread(way, c, gap))
            turn = 1 - 2 * way
            for gap in range(1, lines):
                plane = line + gap * turn
                left((inside(plane), relay_copy(way, c, plane, me + turn * members)))


def layer(summed, gain, named, w_in, w_out, lines, planes, owners, capacity, chunks):
    tokens, width = summed.shape
    members = planes * owners
    cols = width // members // chunks
    places = lines * members
    group = members * tokens
    slots = slots_of(capacity)
    units = w_in.shape[1]
    spans, pieces = 4, 8
    f32, bf16 = jnp.float32, jnp.bfloat16
    vmem = pl.BlockSpec(memory_space=pltpu.VMEM)
    hbm = pl.BlockSpec(memory_space=pl.ANY)
    dma = pltpu.SemaphoreType.DMA
    return pl.pallas_call(
        functools.partial(layer_kernel, (lines, planes, owners, chunks, capacity)),
        out_shape=jax.ShapeDtypeStruct((tokens, width), bf16),
        in_specs=[vmem, vmem, vmem, hbm, hbm],
        out_specs=vmem,
        scratch_shapes=[
            pltpu.VMEM(w_in.shape, bf16),
            pltpu.VMEM(w_out.shape, bf16),
            pltpu.VMEM((tokens, 128), f32),
            pltpu.VMEM((tokens, 128), f32),
            pltpu.VMEM((places,) + named.shape, f32),
            pltpu.VMEM((members, chunks, tokens, cols), bf16),
            pltpu.VMEM((chunks, lines * group, cols), bf16),
            pltpu.VMEM((planes * slots, lines * group), bf16),
            pltpu.VMEM((lines, group, planes * slots), bf16),
            pltpu.VMEM((planes * slots, 128), f32),
            pltpu.VMEM((chunks, planes, capacity, cols), bf16),
            pltpu.VMEM((chunks, capacity, members * cols), bf16),
            pltpu.VMEM((capacity, units), f32),
            pltpu.VMEM((spans, capacity, units // spans), bf16),
            pltpu.VMEM((spans, capacity, units // spans), bf16),
            pltpu.VMEM((capacity, units), bf16),
            pltpu.VMEM((chunks, members - 1, capacity, cols), bf16),
            pltpu.VMEM((chunks, members, capacity, cols), bf16),
            pltpu.VMEM((chunks, planes * slots, cols), bf16),
            pltpu.VMEM((2, chunks, lines, group, cols), bf16),
            pltpu.VMEM((2, chunks, lines, group, cols), bf16),
            pltpu.VMEM((chunks, group, cols), bf16),
            pltpu.VMEM((chunks, members, tokens, cols), bf16),
            dma((chunks, members)),
            dma((pieces,)),
            dma((2,)),
            dma((2, places)),
            dma((2, chunks, members)),
            dma((2, 2, chunks, lines)),
            dma((2, chunks, members)),
            dma((2, spans)),
            dma((2, chunks, members)),
            dma((2, 2, chunks, lines)),
            dma((2, chunks, members)),
        ],
        compiler_params=pltpu.CompilerParams(
            collective_id=3, has_side_effects=True, vmem_limit_bytes=63 * 1024 * 1024
        ),
    )(summed, gain, named, w_in, w_out)


def planes_of(places, tokens, width, units, capacity):
    owners, rest = divmod(places, EXPERTS)
    planes = 2
    members = planes * owners
    if rest or lax.axis_size("tensor") != 2 or members < 2 or members * tokens != 128:
        return 0
    if width % (members * 128) or units % 2048 or capacity % 16:
        return 0
    held = 4 * units * width + 12 * capacity * units
    return planes if held < 56 * 1024 * 1024 else 0


def named_tile(expert_ids, expert_weights, members):
    tokens = expert_ids.shape[0]
    spot = lax.rem(lax.axis_index("dp"), members)
    rows = jnp.concatenate([expert_ids.astype(jnp.float32), expert_weights], axis=1).T
    rows = jnp.tile(rows, (1, members))
    here = jnp.arange(members * tokens, dtype=jnp.int32)[None, :] // tokens == spot
    return jnp.pad(jnp.where(here, rows, 0.0), ((0, 8 - rows.shape[0]), (0, 0)))


def shards(
    residual, queries, keys, values, lengths, norm_gain, expert_ids, expert_weights, w_in, w_out
):
    tokens = residual.shape[0]
    width_local = residual.shape[1]
    head_groups = keys.shape[2] // HEAD
    group_size = HEADS // KV
    query_rows = queries.reshape(tokens, head_groups, group_size, HEAD)
    key_rows = keys.reshape(tokens, CACHE, head_groups, HEAD)
    value_rows = values.reshape(tokens, CACHE, head_groups, HEAD)
    scores = jnp.einsum(
        "tgjd,tlgd->tgjl", query_rows, key_rows, preferred_element_type=jnp.float32
    ) * HEAD ** (-0.5)
    live_mask = (jnp.arange(CACHE, dtype=jnp.int32)[None, :] < lengths[:, None])[:, None, None, :]
    scores = jnp.where(live_mask, scores, -1e30)
    peak_score = jnp.max(scores, axis=-1, keepdims=True)
    powered = jnp.exp(scores - peak_score)
    attention_probs = (powered / jnp.sum(powered, axis=-1, keepdims=True)).astype(jnp.bfloat16)
    attended = jnp.einsum(
        "tgjl,tlgd->tgjd", attention_probs, value_rows, preferred_element_type=jnp.float32
    )
    summed = residual.astype(jnp.float32) + attended.reshape(tokens, width_local)
    places = lax.axis_size("dp")
    capacity = tokens * places * TOPK * 3 // (4 * EXPERTS)
    planes = planes_of(places, tokens, width_local, w_in.shape[1], capacity)
    if planes:
        owners = places // EXPERTS
        return layer(
            summed, norm_gain[None, :], named_tile(expert_ids, expert_weights, planes * owners),
            w_in, w_out, EXPERTS // planes, planes, owners, capacity, 3,
        )
    square_sums = lax.psum(jnp.sum(summed * summed, axis=1), "tensor")
    normed = (
        summed
        * lax.rsqrt(square_sums[:, None] / D + NORM_EPSILON)
        * norm_gain.astype(jnp.float32)[None, :]
    ).astype(jnp.bfloat16)
    flat_ids = expert_ids.reshape(-1)
    expert_iota = jnp.arange(EXPERTS, dtype=jnp.int32)
    onehot = (flat_ids[:, None] == expert_iota[None, :]).astype(jnp.int32)
    local_rank = jnp.sum(
        (jnp.cumsum(onehot, axis=0, dtype=jnp.int32) - onehot) * onehot, axis=1, dtype=jnp.int32
    )
    counts = jnp.sum(onehot, axis=0, dtype=jnp.int32)
    me = lax.axis_index("dp")
    owners = places // EXPERTS
    slot_total = EXPERTS * SRC_CAP
    pair_target = flat_ids * SRC_CAP + local_rank
    pick_pairs = pair_target[None, :] == jnp.arange(slot_total, dtype=jnp.int32)[:, None]
    pick_tokens = jnp.sum(
        pick_pairs.reshape(slot_total, tokens, TOPK).astype(jnp.float32), axis=2
    ).astype(jnp.bfloat16)
    packed = jnp.dot(pick_tokens, normed, preferred_element_type=jnp.float32).astype(jnp.bfloat16)
    padded_counts = jnp.pad(counts[None, :], ((0, 0), (0, 128 - EXPERTS)))
    received, gathered = dispatch(
        packed.reshape(EXPERTS, SRC_CAP, width_local), padded_counts, owners
    )
    all_counts = gathered[:, 0, :EXPERTS]
    place_iota = jnp.arange(places, dtype=jnp.int32)
    offsets = jnp.sum(jnp.where(place_iota[:, None] < me, all_counts, 0), axis=0, dtype=jnp.int32)
    slot_index = local_rank + jnp.sum(onehot * offsets[None, :], axis=1, dtype=jnp.int32)
    keep_mask = slot_index < capacity
    mine = jnp.sum(
        jnp.where(expert_iota[None, :] == me // owners, all_counts, 0), axis=1, dtype=jnp.int32
    )
    before = jnp.sum(
        jnp.where(place_iota[None, :] < place_iota[:, None], mine[None, :], 0),
        axis=1,
        dtype=jnp.int32,
    )
    rank = jnp.arange(SRC_CAP, dtype=jnp.int32)[None, :]
    row_slot = jnp.where(rank < mine[:, None], before[:, None] + rank, -1).reshape(-1)
    pick_rows = (
        row_slot[None, :] == jnp.arange(capacity, dtype=jnp.int32)[:, None]
    ).astype(jnp.bfloat16)
    total_rows = places * SRC_CAP
    compact = jnp.dot(
        pick_rows, received.reshape(total_rows, width_local), preferred_element_type=jnp.float32
    ).astype(jnp.bfloat16)
    results = expert_rows(compact, w_in, w_out).astype(jnp.bfloat16)
    spread = jnp.einsum(
        "cr,cd->rd", pick_rows, results, preferred_element_type=jnp.float32
    ).astype(jnp.bfloat16)
    per_expert = (
        send_back(spread.reshape(places, SRC_CAP, width_local), owners)
        .reshape(slot_total, width_local)
        .astype(jnp.float32)
    )
    pair_weight = expert_weights.reshape(-1) * keep_mask.astype(jnp.float32)
    mix_rows = jnp.sum(
        (pick_pairs.astype(jnp.float32) * pair_weight[None, :]).reshape(slot_total, tokens, TOPK),
        axis=2,
    )
    addition = jnp.einsum("st,sd->td", mix_rows, per_expert, precision=lax.Precision.HIGHEST)
    return (summed + addition).astype(jnp.bfloat16)


def solution(mesh):
    in_specs = (
        P("dp", "tensor"),
        P("dp", "tensor"),
        P("dp", None, "tensor"),
        P("dp", None, "tensor"),
        P("dp"),
        P("tensor"),
        P("dp", None),
        P("dp", None),
        P("tensor", "dp"),
        P("dp", "tensor"),
    )
    out_specs = P("dp", "tensor")
    return jax.shard_map(shards, mesh=mesh, in_specs=in_specs, out_specs=out_specs, check_vma=False)
```

```python
import functools

import jax
import jax.numpy as jnp
from jax import lax
from jax.experimental import pallas as pl
from jax.experimental.pallas import tpu as pltpu
from jax.sharding import PartitionSpec as P

D = 6144
HEADS = 48
KV = 8
HEAD = 128
EXPERTS = 8
TOPK = 2
CACHE = 128
SRC_CAP = 16


NORM_EPSILON = 1e-05


MESH = pl.DeviceIdType.MESH


def remote(source, target, send_sem, recv_sem, place):
    return pltpu.make_async_remote_copy(
        src_ref=source,
        dst_ref=target,
        send_sem=send_sem,
        recv_sem=recv_sem,
        device_id={"dp": place},
        device_id_type=MESH,
    )


def greet(places):
    barrier = pltpu.get_barrier_semaphore()
    for place in places:
        pl.semaphore_signal(barrier, inc=1, device_id={"dp": place}, device_id_type=MESH)
    pl.semaphore_wait(barrier, len(places))


def far_first(amount):
    return sorted(range(1, amount), key=lambda lap: (-min(lap, amount - lap), lap))


def dispatch_kernel(owners, packed, counts, received, all_counts, plane_send, plane_recv,
                    pair_send, pair_recv, count_send, count_recv, own_sem):
    experts = packed.shape[0]
    places = experts * owners
    me = lax.axis_index("dp")
    expert, owner = lax.div(me, owners), lax.rem(me, owners)
    greet([lax.rem(me + lap, places) for lap in range(1, places)])
    waiting = []
    for lap in range(1, places):
        copy = remote(counts, all_counts.at[me], count_send.at[lap], count_recv.at[lap],
                      lax.rem(me + lap, places))
        copy.start()
        waiting.append(copy)
    own = pltpu.make_async_copy(packed.at[expert], received.at[me], own_sem)
    own.start()
    own_count = pltpu.make_async_copy(counts, all_counts.at[me], count_recv.at[0])
    own_count.start()

    def forward(source, place, lap):
        for step in range(1, owners):
            other = lax.rem(owner + step, owners)
            spot = lap * owners + step
            copy = remote(source, received.at[place], pair_send.at[spot], pair_recv.at[spot],
                          expert * owners + other)
            copy.start()
            waiting.append(copy)

    forward(packed.at[expert], me, 0)
    middle = far_first(experts)
    order = [lap for lap in middle if lap in (1, experts - 1)]
    order += [lap for lap in middle if lap not in (1, experts - 1)]
    for lap in order:
        target = lax.rem(expert + lap, experts)
        copy = remote(packed.at[target], received.at[me], plane_send.at[lap], plane_recv.at[lap],
                      target * owners + owner)
        copy.start()
        waiting.append(copy)
    for lap in order:
        source = lax.rem(expert + experts - lap, experts) * owners + owner
        remote(received.at[source], received.at[source], plane_send.at[lap], plane_recv.at[lap],
               source).wait_recv()
        forward(received.at[source], source, lap)
    for lap in [0] + order:
        for step in range(1, owners):
            other = lax.rem(owner + owners - step, owners)
            place = lax.rem(expert + experts - lap, experts) * owners + other
            spot = lap * owners + step
            remote(received.at[place], received.at[place], pair_send.at[spot], pair_recv.at[spot],
                   expert * owners + other).wait_recv()
    for lap in range(1, places):
        source = lax.rem(me + places - lap, places)
        remote(counts, all_counts.at[source], count_send.at[lap], count_recv.at[lap],
               source).wait_recv()
    own.wait()
    own_count.wait()
    for copy in waiting:
        copy.wait_send()


def dispatch(packed, counts, owners):
    experts, rows, width = packed.shape
    places = experts * owners
    dma = pltpu.SemaphoreType.DMA
    vmem = pl.BlockSpec(memory_space=pltpu.VMEM)
    return pl.pallas_call(
        functools.partial(dispatch_kernel, owners),
        out_shape=(
            jax.ShapeDtypeStruct((places, rows, width), packed.dtype),
            jax.ShapeDtypeStruct((places,) + counts.shape, counts.dtype),
        ),
        in_specs=[vmem, vmem],
        out_specs=(vmem, vmem),
        scratch_shapes=[
            dma((experts,)),
            dma((experts,)),
            dma((places,)),
            dma((places,)),
            dma((places,)),
            dma((places,)),
            dma,
        ],
        compiler_params=pltpu.CompilerParams(collective_id=0, has_side_effects=True),
    )(packed, counts)


def return_kernel(owners, part, out, landed, total, pair_send, pair_recv, plane_send, plane_recv):
    experts = out.shape[0]
    me = lax.axis_index("dp")
    expert, owner = lax.div(me, owners), lax.rem(me, owners)
    greet(
        [lax.rem(expert + lap, experts) * owners + owner for lap in range(1, experts)]
        + [expert * owners + lax.rem(owner + step, owners) for step in range(1, owners)]
    )
    order = far_first(experts) + [0]
    waiting = []
    for lap in order:
        for step in range(1, owners):
            other = lax.rem(owner + step, owners)
            source = lax.rem(expert + lap, experts) * owners + other
            spot = lap * owners + step
            copy = remote(part.at[source], landed.at[spot], pair_send.at[spot], pair_recv.at[spot],
                          expert * owners + other)
            copy.start()
            waiting.append(copy)
    for lap in order:
        target = lax.rem(expert + lap, experts) * owners + owner
        value = part[target].astype(jnp.float32)
        for step in range(1, owners):
            other = lax.rem(owner + owners - step, owners)
            spot = lap * owners + step
            remote(landed.at[spot], landed.at[spot], pair_send.at[spot], pair_recv.at[spot],
                   expert * owners + other).wait_recv()
            value += landed[spot].astype(jnp.float32)
        if lap == 0:
            out[expert] = value.astype(out.dtype)
        else:
            total[lap] = value.astype(total.dtype)
            copy = remote(total.at[lap], out.at[expert], plane_send.at[lap], plane_recv.at[lap],
                          target)
            copy.start()
            waiting.append(copy)
    for lap in order[:-1]:
        source = lax.rem(expert + experts - lap, experts)
        remote(total.at[lap], out.at[source], plane_send.at[lap], plane_recv.at[lap],
               source * owners + owner).wait_recv()
    for copy in waiting:
        copy.wait_send()


def send_back(part, owners):
    places, rows, width = part.shape
    experts = places // owners
    dma = pltpu.SemaphoreType.DMA
    vmem = pl.BlockSpec(memory_space=pltpu.VMEM)
    return pl.pallas_call(
        functools.partial(return_kernel, owners),
        out_shape=jax.ShapeDtypeStruct((experts, rows, width), part.dtype),
        in_specs=[vmem],
        out_specs=vmem,
        scratch_shapes=[
            pltpu.VMEM((places, rows, width), part.dtype),
            pltpu.VMEM((experts, rows, width), part.dtype),
            dma((places,)),
            dma((places,)),
            dma((experts,)),
            dma((experts,)),
        ],
        compiler_params=pltpu.CompilerParams(collective_id=1, has_side_effects=True),
    )(part)


def hidden_kernel(members, chunk, part, out, landed, send_sem, recv_sem):
    me = lax.axis_index("tensor")
    barrier = pltpu.get_barrier_semaphore()
    for step in range(1, members):
        pl.semaphore_signal(
            barrier,
            inc=1,
            device_id={"tensor": lax.rem(me + step, members)},
            device_id_type=MESH,
        )
    pl.semaphore_wait(barrier, members - 1)

    def piece_copy(piece, step):
        rows = pl.ds(piece * chunk, chunk)
        spot = piece * members + step
        return pltpu.make_async_remote_copy(
            src_ref=part.at[rows],
            dst_ref=landed.at[step, rows],
            send_sem=send_sem.at[spot],
            recv_sem=recv_sem.at[spot],
            device_id={"tensor": lax.rem(me + step, members)},
            device_id_type=MESH,
        )

    copies = [
        [piece_copy(piece, step) for step in range(1, members)]
        for piece in range(part.shape[0] // chunk)
    ]
    for row in copies:
        for copy in row:
            copy.start()
    for piece, row in enumerate(copies):
        rows = pl.ds(piece * chunk, chunk)
        value = part[rows].astype(jnp.float32)
        for step, copy in enumerate(row, 1):
            copy.wait_recv()
            value += landed[step, rows].astype(jnp.float32)
        out[rows] = (value / (1.0 + jnp.exp(-value))).astype(out.dtype)
    for row in copies:
        for copy in row:
            copy.wait_send()


def hidden_rows(part):
    members = lax.axis_size("tensor")
    rows = part.shape[0]
    chunk = 32 if rows % 32 == 0 else rows
    dma = pltpu.SemaphoreType.DMA
    vmem = pl.BlockSpec(memory_space=pltpu.VMEM)
    return pl.pallas_call(
        functools.partial(hidden_kernel, members, chunk),
        out_shape=jax.ShapeDtypeStruct(part.shape, part.dtype),
        in_specs=[vmem],
        out_specs=vmem,
        scratch_shapes=[
            pltpu.VMEM((members,) + part.shape, part.dtype),
            dma((members * (rows // chunk),)),
            dma((members * (rows // chunk),)),
        ],
        compiler_params=pltpu.CompilerParams(collective_id=2, has_side_effects=True),
    )(part)


def expert_rows(tok_rows, w_in, w_out):
    partial_sum = jnp.einsum("rd,df->rf", tok_rows, w_in, preferred_element_type=jnp.float32)
    hidden = hidden_rows(partial_sum.astype(jnp.bfloat16))
    return jnp.einsum("rf,fd->rd", hidden, w_out, preferred_element_type=jnp.float32)


def slots_of(rows):
    return -(-rows // 128) * 128


def layer_kernel(dims, residual, queries, keys, values, lengths, gain, names, shares, w_in, w_out,
                 out, win, wout, summed, heads, named, squares, squares_in, gath, nrm, tok, pick, pick_t, slot_weight, sendx, gotx, acc, part, part_in, hidden,
                 sendy, goty, weighted, line_out, line_in, fin, extra,
                 kv_sem, in_sem, out_sem, sq_sem, gath_sem, first_sem, line_sem, third_sem, part_sem,
                 back_sem, relay_sem, home_sem):
    lines, planes, owners, chunks, capacity = dims
    tokens, width = residual.shape
    members = planes * owners
    places = lines * members
    quarter = width // members
    cols = quarter // chunks
    group = members * tokens
    slots = slots_of(capacity)
    units = w_in.shape[1]
    me = lax.axis_index("dp")
    line, spot = lax.div(me, members), lax.rem(me, members)
    own_plane = lax.div(spot, owners)
    other_core = 1 - lax.axis_index("tensor")
    f32, bf16 = jnp.float32, jnp.bfloat16

    def far(source, target, send, recv, device):
        return pltpu.make_async_remote_copy(
            src_ref=source, dst_ref=target, send_sem=send, recv_sem=recv, device_id=device,
            device_id_type=MESH,
        )

    def arrived(shape_like, recv):
        far(shape_like, shape_like, recv, recv, {"tensor": other_core}).wait_recv()

    def departed(shape_like, send):
        far(shape_like, shape_like, send, send, {"tensor": other_core}).wait_send()

    def peer(step):
        return lax.rem(spot + step, members)

    def sender(step):
        return lax.rem(spot + members - step, members)

    def place(index):
        return {"dp": line * members + index}

    steps = range(1, members)
    last = members - 1
    depth = members * cols
    width_kv = keys.shape[1]
    cache = keys.shape[0] // tokens
    per_kv = width_kv // HEAD
    per_group = HEADS // KV
    count = width // HEAD
    batches = kv_sem.shape[0]
    batch = tokens // batches

    def kv_copies(i):
        rows = pl.ds(i * batch * cache, batch * cache)
        return [
            pltpu.make_async_copy(keys.at[rows], wout.at[rows, pl.ds(0, width_kv)], kv_sem.at[i]),
            pltpu.make_async_copy(
                values.at[rows], wout.at[rows, pl.ds(width_kv, width_kv)], kv_sem.at[i]
            ),
        ]

    def win_copy(i):
        c, q = lax.div(i, members), lax.rem(i, members)
        return pltpu.make_async_copy(
            w_in.at[pl.ds(pl.multiple_of(q * quarter + c * cols, cols), cols)],
            win.at[pl.ds(pl.multiple_of(i * cols, cols), cols)],
            in_sem.at[c],
        )

    pieces = 8
    piece = units // pieces
    wout_copies = [
        pltpu.make_async_copy(
            w_out.at[pl.ds(i * piece, piece)], wout.at[pl.ds(i * piece, piece)], out_sem.at[0]
        )
        for i in range(pieces)
    ]
    barrier = pltpu.get_barrier_semaphore()
    for lap in range(1, places):
        pl.semaphore_signal(
            barrier, inc=1, device_id={"dp": lax.rem(me + lap, places)}, device_id_type=MESH
        )
    pl.semaphore_signal(barrier, inc=1, device_id={"tensor": other_core}, device_id_type=MESH)
    for i in range(batches):
        for copy in kv_copies(i):
            copy.start()
    lane = lax.broadcasted_iota(jnp.int32, (8, group), 1)
    here = (lane >= spot * tokens) & (lane < spot * tokens + tokens)
    labels = jnp.concatenate([names[...].astype(f32), shares[...], jnp.zeros((4, tokens), f32)], axis=0)
    named[...] = jnp.where(here, jnp.concatenate([labels] * members, axis=1), 0.0)
    for h in range(count):
        heads[pl.ds(h, tokens, stride=count)] = queries[:, h * HEAD:(h + 1) * HEAD].astype(f32)
    head_row = lax.broadcasted_iota(jnp.int32, (count, HEAD), 0)
    owned = [
        (head_row >= g * per_group) & (head_row < (g + 1) * per_group) for g in range(per_kv)
    ]
    position = lax.broadcasted_iota(jnp.int32, (count, cache), 1)
    feeds = -(-members * chunks // batches)

    @pl.loop(0, batches)
    def _(i):
        rows = pl.ds(i * batch * cache, batch * cache)
        whole = wout.at[rows, pl.ds(0, 2 * width_kv)]
        pltpu.make_async_copy(w_out.at[pl.ds(0, batch * cache), pl.ds(0, 2 * width_kv)], whole,
                              kv_sem.at[i]).wait()
        for k in range(feeds):
            @pl.when(i * feeds + k < members * chunks)
            def _():
                win_copy(i * feeds + k).start()
        probs = []
        for j in range(batch):
            t = i * batch + j
            query = heads[pl.ds(pl.multiple_of(t * count, 8), count)]
            query = jnp.concatenate(
                [jnp.where(mask, query, 0.0) for mask in owned], axis=1
            ).astype(bf16)
            key = wout[pl.ds(pl.multiple_of(t * cache, cache), cache), 0:width_kv]
            score = lax.dot_general(query, key, (((1,), (1,)), ((), ())),
                                    preferred_element_type=f32) * HEAD ** (-0.5)
            score = jnp.where(position < lengths[t], score, -1e30)
            powered = jnp.exp(score - jnp.max(score, axis=1, keepdims=True))
            probs.append(
                (powered / jnp.sum(powered, axis=1, keepdims=True)).astype(bf16)
            )
        for j in range(batch):
            t = i * batch + j
            value = wout[pl.ds(pl.multiple_of(t * cache, cache), cache), width_kv:2 * width_kv]
            mixed = jnp.dot(probs[j], value, preferred_element_type=f32)
            attended = jnp.where(owned[0], mixed[:, 0:HEAD], 0.0)
            for g in range(1, per_kv):
                attended += jnp.where(owned[g], mixed[:, g * HEAD:(g + 1) * HEAD], 0.0)
            heads[pl.ds(pl.multiple_of(t * count, 8), count)] = attended

    for copy in wout_copies:
        copy.start()
    total = jnp.zeros((tokens, 1), f32)
    for h in range(count):
        at = h * HEAD
        value = residual[:, at:at + HEAD].astype(f32) + heads[pl.ds(h, tokens, stride=count)]
        summed[:, at:at + HEAD] = value
        total += jnp.sum(value * value, axis=1, keepdims=True)
    squares[...] = jnp.broadcast_to(total, squares.shape)
    pl.semaphore_wait(barrier, places)
    square_copy = far(squares, squares_in, sq_sem.at[0], sq_sem.at[1], {"tensor": other_core})
    square_copy.start()
    for lap in range(1, places):
        far(named, gath.at[me], gath_sem.at[0], gath_sem.at[1],
            {"dp": lax.rem(me + lap, places)}).start()
    gath[me] = named[...]
    square_copy.wait_recv()
    scale = lax.rsqrt(
        (squares[:, :1] + squares_in[:, :1]) / (2 * width) + NORM_EPSILON
    )
    for c in range(chunks):
        for q in range(members):
            at = q * quarter + c * cols
            nrm[q, c] = (
                summed[:, at:at + cols] * scale * gain[:, at:at + cols].astype(f32)
            ).astype(bf16)
        home = pl.ds(pl.multiple_of(line * group + spot * tokens, tokens), tokens)
        tok[c, home] = nrm[spot, c]
        for step in steps:
            far(nrm.at[peer(step), c], tok.at[c, home], first_sem.at[chunks], first_sem.at[c],
                place(peer(step))).start()

    def rows_of(plane):
        return pl.ds(pl.multiple_of(plane * group, group), group)

    def inside(plane):
        return (plane >= 0) & (plane < lines)

    def spread(way, c, gap):
        turn = 1 - 2 * way
        plane = line - gap * turn
        rows = rows_of(plane)
        return inside(plane) & inside(line + turn), far(
            tok.at[c, rows], tok.at[c, rows], line_sem.at[2 * chunks * lines + way],
            line_sem.at[(way * chunks + c) * lines + plane], {"dp": me + turn * members},
        )

    def arrive(way, c, gap):
        plane = line - gap * (1 - 2 * way)

        @pl.when(inside(plane))
        def _():
            arrived(tok.at[c, rows_of(plane)], line_sem.at[(way * chunks + c) * lines + plane])

    def begin(pair):
        @pl.when(pair[0])
        def _():
            pair[1].start()

    for c in range(chunks):
        arrived(nrm.at[pl.ds(0, last), c], first_sem.at[c])
        for way in (0, 1):
            begin(spread(way, c, 0))

    arrived(gath.at[pl.ds(0, places - 1)], gath_sem.at[1])
    hits, weights = [], []
    for p in range(lines):
        tile = gath[p * members]
        for m in range(1, members):
            tile += gath[p * members + m]
        for b in range(planes):
            expert = (line * planes + b).astype(f32)
            first, second = tile[0:1] == expert, tile[1:2] == expert
            hits.append(jnp.where(first | second, 1.0, 0.0))
            weights.append(jnp.where(first, tile[2:3], jnp.where(second, tile[3:4], 0.0)))
    earlier = lax.broadcasted_iota(jnp.int32, (group, group), 0)
    later = lax.broadcasted_iota(jnp.int32, (group, group), 1)
    before = jnp.where(earlier < later, 1.0, 0.0).astype(bf16)
    slot_iota = lax.broadcasted_iota(jnp.int32, (slots, group), 0).astype(f32)
    for b in range(planes):
        offset = jnp.zeros((1, 1), f32)
        slot_total = jnp.zeros((slots, 1), f32)
        for p in range(lines):
            hit, weight = hits[p * planes + b], weights[p * planes + b]
            wide = jnp.broadcast_to(hit, (16, group)).astype(bf16)
            rank = jnp.dot(wide, before, preferred_element_type=f32)[0:1] + offset
            offset += jnp.sum(hit, axis=1, keepdims=True)
            rank = jnp.where((hit > 0.0) & (rank < capacity), rank, -1.0)
            chosen = jnp.where(slot_iota == rank, 1.0, 0.0)
            pick[b * slots:(b + 1) * slots, p * group:(p + 1) * group] = chosen.astype(bf16)
            pick_t[p, :, b * slots:(b + 1) * slots] = chosen.T.astype(bf16)
            slot_total += jnp.sum(chosen * weight, axis=1, keepdims=True)
        slot_weight[b * slots:(b + 1) * slots] = jnp.broadcast_to(slot_total, (slots, 128))
    weighted[...] = jnp.zeros_like(weighted)

    def lanes_of(index):
        return pl.ds(pl.multiple_of(index * cols, 128), cols)

    block = 512
    spans = part.shape[0]
    span = units // spans

    def product(c, at):
        at = pl.multiple_of(at, 128)
        return jnp.dot(gotx[c], win[c * depth:(c + 1) * depth, pl.ds(at, block)],
                       preferred_element_type=f32)

    def expand(c):
        arrived(goty.at[c, pl.ds(0, last)], third_sem.at[c])
        pltpu.make_async_copy(w_in.at[pl.ds(0, depth)], win.at[pl.ds(c * depth, depth)],
                              in_sem.at[c]).wait()
        if c < chunks - 1:
            @pl.loop(0, units // block)
            def _(i):
                at = pl.multiple_of(i * block, block)
                value = product(c, at)
                acc[:, pl.ds(at, block)] = value if c == 0 else acc[:, pl.ds(at, block)] + value
            return
        for h in range(spans):
            @pl.loop(0, span // block)
            def _(i):
                inner = pl.multiple_of(i * block, block)
                at = h * span + inner
                value = product(c, at)
                if c:
                    value += acc[:, pl.ds(pl.multiple_of(at, block), block)]
                part[h, :, pl.ds(inner, block)] = value.astype(bf16)
            far(part.at[h], part_in.at[h], part_sem.at[spans], part_sem.at[h],
                {"tensor": other_core}).start()

    for c in range(chunks):
        for gap in range(1, lines):
            for way in (0, 1):
                arrive(way, c, gap)
                begin(spread(way, c, gap))
        rows = jnp.dot(pick[...], tok[c], preferred_element_type=f32).astype(bf16)
        for b in range(planes):
            sendx[c, b] = rows[b * slots:b * slots + capacity]
        for step in steps:
            far(sendx.at[c, lax.div(peer(step), owners)], gotx.at[c, :, lanes_of(spot)],
                third_sem.at[chunks], third_sem.at[c], place(peer(step))).start()
        gotx[c, :, lanes_of(spot)] = sendx[c, own_plane]
        if c:
            expand(c - 1)
    expand(chunks - 1)
    for h in range(spans):
        arrived(part_in.at[h], part_sem.at[h])

        @pl.loop(0, span // block)
        def _(i):
            at = pl.ds(pl.multiple_of(i * block, block), block)
            value = part[h, :, at].astype(f32) + part_in[h, :, at].astype(f32)
            value = value / (1.0 + jnp.exp(-value))
            hidden[:, pl.ds(pl.multiple_of(h * span + i * block, block), block)] = (
                value.astype(bf16)
            )
    pltpu.make_async_copy(w_out, wout, out_sem.at[0]).wait()

    def contract(c):
        for step in list(steps) + [0]:
            at = pl.multiple_of(peer(step) * quarter + c * cols, 128)
            value = jnp.dot(hidden[...], wout[:, pl.ds(at, cols)], preferred_element_type=f32)
            if step:
                sendy[c, step - 1] = value.astype(bf16)
                far(sendy.at[c, step - 1], goty.at[c, spot], back_sem.at[chunks], back_sem.at[c],
                    place(peer(step))).start()
            else:
                goty[c, spot] = value.astype(bf16)

    def gather_back(c):
        arrived(sendy.at[c], back_sem.at[c])
        for b in range(planes):
            value = goty[c, b * owners].astype(f32)
            for o in range(1, owners):
                value += goty[c, b * owners + o].astype(f32)
            value = value * slot_weight[b * slots:b * slots + capacity, :1]
            weighted[c, b * slots:b * slots + capacity] = value.astype(bf16)

    def share(c, plane):
        return jnp.dot(pick_t[plane], weighted[c], preferred_element_type=f32)

    def relay_mark(way, c, plane):
        return relay_sem.at[(way * chunks + c) * lines + plane]

    def relay(way, c, gap):
        turn = 1 - 2 * way
        plane = line + gap * turn

        @pl.when(inside(plane))
        def _():
            value = share(c, plane)
            line_out[way, c, plane] = value.astype(bf16)

            @pl.when(inside(line - turn))
            def _():
                arrived(line_in.at[way, c, plane], relay_mark(way, c, plane))
                line_out[way, c, plane] = (
                    value + line_in[way, c, plane].astype(f32)
                ).astype(bf16)

            far(line_out.at[way, c, plane], line_in.at[way, c, plane],
                relay_sem.at[2 * chunks * lines + way], relay_mark(way, c, plane),
                {"dp": me + turn * members}).start()

    near = jnp.where(line * 2 < lines, 0, 1)

    def finish(c):
        for way in (0, 1):
            turn = 1 - 2 * way

            @pl.when(inside(line - turn))
            def _():
                arrived(line_in.at[way, c, line], relay_mark(way, c, line))

        low, high = line > 0, line < lines - 1

        def got(way):
            return line_in[way, c, line].astype(f32)

        @pl.when(low & high)
        def _():
            fin[c] = (share(c, line) + got(0) + got(1)).astype(bf16)

        @pl.when(low & ~high)
        def _():
            fin[c] = (share(c, line) + got(0)).astype(bf16)

        @pl.when(high & ~low)
        def _():
            fin[c] = (share(c, line) + got(1)).astype(bf16)

        for step in steps:
            rows = pl.ds(pl.multiple_of(peer(step) * tokens, tokens), tokens)
            far(fin.at[c, rows], extra.at[c, spot], home_sem.at[chunks], home_sem.at[c],
                place(peer(step))).start()
        extra[c, spot] = fin[c, pl.ds(pl.multiple_of(spot * tokens, tokens), tokens)]

    def close(c):
        arrived(extra.at[c, pl.ds(0, last)], home_sem.at[c])
        for q in range(members):
            at = q * quarter + c * cols
            out[:, at:at + cols] = (
                summed[:, at:at + cols] + extra[c, q].astype(f32)
            ).astype(out.dtype)

    for c in range(chunks):
        contract(c)
        if c:
            gather_back(c - 1)
            for gap in range(lines - 1, 1, -1):
                relay(near, c - 1, gap)
    gather_back(chunks - 1)
    for gap in range(lines - 1, 1, -1):
        relay(near, chunks - 1, gap)
    for c in range(chunks):
        relay(near, c, 1)
    for c in range(chunks):
        for gap in range(lines - 1, 0, -1):
            relay(1 - near, c, gap)
    for c in range(chunks):
        finish(c)
        if c:
            close(c - 1)
    close(chunks - 1)
    departed(squares, sq_sem.at[0])
    departed(gath.at[pl.ds(0, places - 1)], gath_sem.at[0])
    departed(nrm.at[pl.ds(0, last)], first_sem.at[chunks])
    departed(goty.at[:, pl.ds(0, last)], third_sem.at[chunks])
    departed(part, part_sem.at[spans])
    departed(sendy, back_sem.at[chunks])
    departed(extra.at[:, pl.ds(0, last)], home_sem.at[chunks])
    base = 2 * chunks * lines
    for at in range(lines):
        @pl.when(line == at)
        def _():
            above, below = lines - 1 - at, at
            if above:
                departed(tok.at[:, pl.ds(0, (below + 1) * group)], line_sem.at[base])
                departed(line_out.at[0, :, pl.ds(0, above)], relay_sem.at[base])
            if below:
                departed(tok.at[:, pl.ds(0, (above + 1) * group)], line_sem.at[base + 1])
                departed(line_out.at[1, :, pl.ds(0, below)], relay_sem.at[base + 1])


def layer(residual, queries, keys, values, lengths, gain, names, shares, w_in, w_out, lines,
          planes, owners, capacity, chunks):
    tokens, width = residual.shape
    members = planes * owners
    cols = width // members // chunks
    places = lines * members
    group = members * tokens
    slots = slots_of(capacity)
    units = w_in.shape[1]
    spans, batches = 4, 4
    f32, bf16 = jnp.float32, jnp.bfloat16
    vmem = pl.BlockSpec(memory_space=pltpu.VMEM)
    hbm = pl.BlockSpec(memory_space=pl.ANY)
    dma = pltpu.SemaphoreType.DMA
    return pl.pallas_call(
        functools.partial(layer_kernel, (lines, planes, owners, chunks, capacity)),
        out_shape=jax.ShapeDtypeStruct((tokens, width), bf16),
        in_specs=[vmem, vmem, hbm, hbm, pl.BlockSpec(memory_space=pltpu.SMEM), vmem, vmem, vmem,
                  hbm, hbm],
        out_specs=vmem,
        scratch_shapes=[
            pltpu.VMEM(w_in.shape, bf16),
            pltpu.VMEM(w_out.shape, bf16),
            pltpu.VMEM((tokens, width), f32),
            pltpu.VMEM((tokens * width // HEAD, HEAD), f32),
            pltpu.VMEM((8, group), f32),
            pltpu.VMEM((tokens, 128), f32),
            pltpu.VMEM((tokens, 128), f32),
            pltpu.VMEM((places, 8, group), f32),
            pltpu.VMEM((members, chunks, tokens, cols), bf16),
            pltpu.VMEM((chunks, lines * group, cols), bf16),
            pltpu.VMEM((planes * slots, lines * group), bf16),
            pltpu.VMEM((lines, group, planes * slots), bf16),
            pltpu.VMEM((planes * slots, 128), f32),
            pltpu.VMEM((chunks, planes, capacity, cols), bf16),
            pltpu.VMEM((chunks, capacity, members * cols), bf16),
            pltpu.VMEM((capacity, units), f32),
            pltpu.VMEM((spans, capacity, units // spans), bf16),
            pltpu.VMEM((spans, capacity, units // spans), bf16),
            pltpu.VMEM((capacity, units), bf16),
            pltpu.VMEM((chunks, members - 1, capacity, cols), bf16),
            pltpu.VMEM((chunks, members, capacity, cols), bf16),
            pltpu.VMEM((chunks, planes * slots, cols), bf16),
            pltpu.VMEM((2, chunks, lines, group, cols), bf16),
            pltpu.VMEM((2, chunks, lines, group, cols), bf16),
            pltpu.VMEM((chunks, group, cols), bf16),
            pltpu.VMEM((chunks, members, tokens, cols), bf16),
            dma((batches,)),
            dma((chunks,)),
            dma((1,)),
            dma((2,)),
            dma((2,)),
            dma((chunks + 1,)),
            dma((2 * chunks * lines + 2,)),
            dma((chunks + 1,)),
            dma((spans + 1,)),
            dma((chunks + 1,)),
            dma((2 * chunks * lines + 2,)),
            dma((chunks + 1,)),
        ],
        compiler_params=pltpu.CompilerParams(
            collective_id=3, has_side_effects=True, vmem_limit_bytes=63 * 1024 * 1024
        ),
    )(residual, queries, keys, values, lengths, gain, names, shares, w_in, w_out)


def planes_of(places, tokens, width, width_kv, units, capacity):
    owners, rest = divmod(places, EXPERTS)
    planes = 2
    members = planes * owners
    if rest or lax.axis_size("tensor") != 2 or members < 2 or members * tokens != 128:
        return 0
    if width % (members * 128) or units % 2048 or capacity % 16:
        return 0
    if tokens * CACHE > units or 2 * width_kv > width or CACHE % 128 or HEAD != 128:
        return 0
    held = 4 * units * width + 12 * capacity * units
    return planes if held < 56 * 1024 * 1024 else 0


def shards(
    residual, queries, keys, values, lengths, norm_gain, expert_ids, expert_weights, w_in, w_out
):
    tokens = residual.shape[0]
    width_local = residual.shape[1]
    places = lax.axis_size("dp")
    capacity = tokens * places * TOPK * 3 // (4 * EXPERTS)
    width_kv = keys.shape[2]
    planes = planes_of(places, tokens, width_local, width_kv, w_in.shape[1], capacity)
    if planes:
        return layer(
            residual, queries, keys.reshape(-1, width_kv), values.reshape(-1, width_kv), lengths,
            norm_gain[None, :], expert_ids.T, expert_weights.T, w_in, w_out, EXPERTS // planes,
            planes, places // EXPERTS, capacity, 3,
        )
    head_groups = keys.shape[2] // HEAD
    group_size = HEADS // KV
    query_rows = queries.reshape(tokens, head_groups, group_size, HEAD)
    key_rows = keys.reshape(tokens, CACHE, head_groups, HEAD)
    value_rows = values.reshape(tokens, CACHE, head_groups, HEAD)
    scores = jnp.einsum(
        "tgjd,tlgd->tgjl", query_rows, key_rows, preferred_element_type=jnp.float32
    ) * HEAD ** (-0.5)
    live_mask = (jnp.arange(CACHE, dtype=jnp.int32)[None, :] < lengths[:, None])[:, None, None, :]
    scores = jnp.where(live_mask, scores, -1e30)
    peak_score = jnp.max(scores, axis=-1, keepdims=True)
    powered = jnp.exp(scores - peak_score)
    attention_probs = (powered / jnp.sum(powered, axis=-1, keepdims=True)).astype(jnp.bfloat16)
    attended = jnp.einsum(
        "tgjl,tlgd->tgjd", attention_probs, value_rows, preferred_element_type=jnp.float32
    )
    summed = residual.astype(jnp.float32) + attended.reshape(tokens, width_local)
    square_sums = lax.psum(jnp.sum(summed * summed, axis=1), "tensor")
    normed = (
        summed
        * lax.rsqrt(square_sums[:, None] / D + NORM_EPSILON)
        * norm_gain.astype(jnp.float32)[None, :]
    ).astype(jnp.bfloat16)
    flat_ids = expert_ids.reshape(-1)
    expert_iota = jnp.arange(EXPERTS, dtype=jnp.int32)
    onehot = (flat_ids[:, None] == expert_iota[None, :]).astype(jnp.int32)
    local_rank = jnp.sum(
        (jnp.cumsum(onehot, axis=0, dtype=jnp.int32) - onehot) * onehot, axis=1, dtype=jnp.int32
    )
    counts = jnp.sum(onehot, axis=0, dtype=jnp.int32)
    me = lax.axis_index("dp")
    owners = places // EXPERTS
    slot_total = EXPERTS * SRC_CAP
    pair_target = flat_ids * SRC_CAP + local_rank
    pick_pairs = pair_target[None, :] == jnp.arange(slot_total, dtype=jnp.int32)[:, None]
    pick_tokens = jnp.sum(
        pick_pairs.reshape(slot_total, tokens, TOPK).astype(jnp.float32), axis=2
    ).astype(jnp.bfloat16)
    packed = jnp.dot(pick_tokens, normed, preferred_element_type=jnp.float32).astype(jnp.bfloat16)
    padded_counts = jnp.pad(counts[None, :], ((0, 0), (0, 128 - EXPERTS)))
    received, gathered = dispatch(
        packed.reshape(EXPERTS, SRC_CAP, width_local), padded_counts, owners
    )
    all_counts = gathered[:, 0, :EXPERTS]
    place_iota = jnp.arange(places, dtype=jnp.int32)
    offsets = jnp.sum(jnp.where(place_iota[:, None] < me, all_counts, 0), axis=0, dtype=jnp.int32)
    slot_index = local_rank + jnp.sum(onehot * offsets[None, :], axis=1, dtype=jnp.int32)
    keep_mask = slot_index < capacity
    mine = jnp.sum(
        jnp.where(expert_iota[None, :] == me // owners, all_counts, 0), axis=1, dtype=jnp.int32
    )
    before = jnp.sum(
        jnp.where(place_iota[None, :] < place_iota[:, None], mine[None, :], 0),
        axis=1,
        dtype=jnp.int32,
    )
    rank = jnp.arange(SRC_CAP, dtype=jnp.int32)[None, :]
    row_slot = jnp.where(rank < mine[:, None], before[:, None] + rank, -1).reshape(-1)
    pick_rows = (
        row_slot[None, :] == jnp.arange(capacity, dtype=jnp.int32)[:, None]
    ).astype(jnp.bfloat16)
    total_rows = places * SRC_CAP
    compact = jnp.dot(
        pick_rows, received.reshape(total_rows, width_local), preferred_element_type=jnp.float32
    ).astype(jnp.bfloat16)
    results = expert_rows(compact, w_in, w_out).astype(jnp.bfloat16)
    spread = jnp.einsum(
        "cr,cd->rd", pick_rows, results, preferred_element_type=jnp.float32
    ).astype(jnp.bfloat16)
    per_expert = (
        send_back(spread.reshape(places, SRC_CAP, width_local), owners)
        .reshape(slot_total, width_local)
        .astype(jnp.float32)
    )
    pair_weight = expert_weights.reshape(-1) * keep_mask.astype(jnp.float32)
    mix_rows = jnp.sum(
        (pick_pairs.astype(jnp.float32) * pair_weight[None, :]).reshape(slot_total, tokens, TOPK),
        axis=2,
    )
    addition = jnp.einsum("st,sd->td", mix_rows, per_expert, precision=lax.Precision.HIGHEST)
    return (summed + addition).astype(jnp.bfloat16)


def solution(mesh):
    in_specs = (
        P("dp", "tensor"),
        P("dp", "tensor"),
        P("dp", None, "tensor"),
        P("dp", None, "tensor"),
        P("dp"),
        P("tensor"),
        P("dp", None),
        P("dp", None),
        P("tensor", "dp"),
        P("dp", "tensor"),
    )
    out_specs = P("dp", "tensor")
    return jax.shard_map(shards, mesh=mesh, in_specs=in_specs, out_specs=out_specs, check_vma=False)
```

```python
import functools

import jax
import jax.numpy as jnp
from jax import lax
from jax.experimental import pallas as pl
from jax.experimental.pallas import tpu as pltpu
from jax.sharding import PartitionSpec as P

D = 6144
HEADS = 48
KV = 8
HEAD = 128
EXPERTS = 8
TOPK = 2
CACHE = 128
SRC_CAP = 16


NORM_EPSILON = 1e-05


MESH = pl.DeviceIdType.MESH


def remote(source, target, send_sem, recv_sem, place):
    return pltpu.make_async_remote_copy(
        src_ref=source,
        dst_ref=target,
        send_sem=send_sem,
        recv_sem=recv_sem,
        device_id={"dp": place},
        device_id_type=MESH,
    )


def greet(places):
    barrier = pltpu.get_barrier_semaphore()
    for place in places:
        pl.semaphore_signal(barrier, inc=1, device_id={"dp": place}, device_id_type=MESH)
    pl.semaphore_wait(barrier, len(places))


def far_first(amount):
    return sorted(range(1, amount), key=lambda lap: (-min(lap, amount - lap), lap))


def dispatch_kernel(owners, packed, counts, received, all_counts, plane_send, plane_recv,
                    pair_send, pair_recv, count_send, count_recv, own_sem):
    experts = packed.shape[0]
    places = experts * owners
    me = lax.axis_index("dp")
    expert, owner = lax.div(me, owners), lax.rem(me, owners)
    greet([lax.rem(me + lap, places) for lap in range(1, places)])
    waiting = []
    for lap in range(1, places):
        copy = remote(counts, all_counts.at[me], count_send.at[lap], count_recv.at[lap],
                      lax.rem(me + lap, places))
        copy.start()
        waiting.append(copy)
    own = pltpu.make_async_copy(packed.at[expert], received.at[me], own_sem)
    own.start()
    own_count = pltpu.make_async_copy(counts, all_counts.at[me], count_recv.at[0])
    own_count.start()

    def forward(source, place, lap):
        for step in range(1, owners):
            other = lax.rem(owner + step, owners)
            spot = lap * owners + step
            copy = remote(source, received.at[place], pair_send.at[spot], pair_recv.at[spot],
                          expert * owners + other)
            copy.start()
            waiting.append(copy)

    forward(packed.at[expert], me, 0)
    middle = far_first(experts)
    order = [lap for lap in middle if lap in (1, experts - 1)]
    order += [lap for lap in middle if lap not in (1, experts - 1)]
    for lap in order:
        target = lax.rem(expert + lap, experts)
        copy = remote(packed.at[target], received.at[me], plane_send.at[lap], plane_recv.at[lap],
                      target * owners + owner)
        copy.start()
        waiting.append(copy)
    for lap in order:
        source = lax.rem(expert + experts - lap, experts) * owners + owner
        remote(received.at[source], received.at[source], plane_send.at[lap], plane_recv.at[lap],
               source).wait_recv()
        forward(received.at[source], source, lap)
    for lap in [0] + order:
        for step in range(1, owners):
            other = lax.rem(owner + owners - step, owners)
            place = lax.rem(expert + experts - lap, experts) * owners + other
            spot = lap * owners + step
            remote(received.at[place], received.at[place], pair_send.at[spot], pair_recv.at[spot],
                   expert * owners + other).wait_recv()
    for lap in range(1, places):
        source = lax.rem(me + places - lap, places)
        remote(counts, all_counts.at[source], count_send.at[lap], count_recv.at[lap],
               source).wait_recv()
    own.wait()
    own_count.wait()
    for copy in waiting:
        copy.wait_send()


def dispatch(packed, counts, owners):
    experts, rows, width = packed.shape
    places = experts * owners
    dma = pltpu.SemaphoreType.DMA
    vmem = pl.BlockSpec(memory_space=pltpu.VMEM)
    return pl.pallas_call(
        functools.partial(dispatch_kernel, owners),
        out_shape=(
            jax.ShapeDtypeStruct((places, rows, width), packed.dtype),
            jax.ShapeDtypeStruct((places,) + counts.shape, counts.dtype),
        ),
        in_specs=[vmem, vmem],
        out_specs=(vmem, vmem),
        scratch_shapes=[
            dma((experts,)),
            dma((experts,)),
            dma((places,)),
            dma((places,)),
            dma((places,)),
            dma((places,)),
            dma,
        ],
        compiler_params=pltpu.CompilerParams(collective_id=0, has_side_effects=True),
    )(packed, counts)


def return_kernel(owners, part, out, landed, total, pair_send, pair_recv, plane_send, plane_recv):
    experts = out.shape[0]
    me = lax.axis_index("dp")
    expert, owner = lax.div(me, owners), lax.rem(me, owners)
    greet(
        [lax.rem(expert + lap, experts) * owners + owner for lap in range(1, experts)]
        + [expert * owners + lax.rem(owner + step, owners) for step in range(1, owners)]
    )
    order = far_first(experts) + [0]
    waiting = []
    for lap in order:
        for step in range(1, owners):
            other = lax.rem(owner + step, owners)
            source = lax.rem(expert + lap, experts) * owners + other
            spot = lap * owners + step
            copy = remote(part.at[source], landed.at[spot], pair_send.at[spot], pair_recv.at[spot],
                          expert * owners + other)
            copy.start()
            waiting.append(copy)
    for lap in order:
        target = lax.rem(expert + lap, experts) * owners + owner
        value = part[target].astype(jnp.float32)
        for step in range(1, owners):
            other = lax.rem(owner + owners - step, owners)
            spot = lap * owners + step
            remote(landed.at[spot], landed.at[spot], pair_send.at[spot], pair_recv.at[spot],
                   expert * owners + other).wait_recv()
            value += landed[spot].astype(jnp.float32)
        if lap == 0:
            out[expert] = value.astype(out.dtype)
        else:
            total[lap] = value.astype(total.dtype)
            copy = remote(total.at[lap], out.at[expert], plane_send.at[lap], plane_recv.at[lap],
                          target)
            copy.start()
            waiting.append(copy)
    for lap in order[:-1]:
        source = lax.rem(expert + experts - lap, experts)
        remote(total.at[lap], out.at[source], plane_send.at[lap], plane_recv.at[lap],
               source * owners + owner).wait_recv()
    for copy in waiting:
        copy.wait_send()


def send_back(part, owners):
    places, rows, width = part.shape
    experts = places // owners
    dma = pltpu.SemaphoreType.DMA
    vmem = pl.BlockSpec(memory_space=pltpu.VMEM)
    return pl.pallas_call(
        functools.partial(return_kernel, owners),
        out_shape=jax.ShapeDtypeStruct((experts, rows, width), part.dtype),
        in_specs=[vmem],
        out_specs=vmem,
        scratch_shapes=[
            pltpu.VMEM((places, rows, width), part.dtype),
            pltpu.VMEM((experts, rows, width), part.dtype),
            dma((places,)),
            dma((places,)),
            dma((experts,)),
            dma((experts,)),
        ],
        compiler_params=pltpu.CompilerParams(collective_id=1, has_side_effects=True),
    )(part)


def hidden_kernel(members, chunk, part, out, landed, send_sem, recv_sem):
    me = lax.axis_index("tensor")
    barrier = pltpu.get_barrier_semaphore()
    for step in range(1, members):
        pl.semaphore_signal(
            barrier,
            inc=1,
            device_id={"tensor": lax.rem(me + step, members)},
            device_id_type=MESH,
        )
    pl.semaphore_wait(barrier, members - 1)

    def piece_copy(piece, step):
        rows = pl.ds(piece * chunk, chunk)
        spot = piece * members + step
        return pltpu.make_async_remote_copy(
            src_ref=part.at[rows],
            dst_ref=landed.at[step, rows],
            send_sem=send_sem.at[spot],
            recv_sem=recv_sem.at[spot],
            device_id={"tensor": lax.rem(me + step, members)},
            device_id_type=MESH,
        )

    copies = [
        [piece_copy(piece, step) for step in range(1, members)]
        for piece in range(part.shape[0] // chunk)
    ]
    for row in copies:
        for copy in row:
            copy.start()
    for piece, row in enumerate(copies):
        rows = pl.ds(piece * chunk, chunk)
        value = part[rows].astype(jnp.float32)
        for step, copy in enumerate(row, 1):
            copy.wait_recv()
            value += landed[step, rows].astype(jnp.float32)
        out[rows] = (value / (1.0 + jnp.exp(-value))).astype(out.dtype)
    for row in copies:
        for copy in row:
            copy.wait_send()


def hidden_rows(part):
    members = lax.axis_size("tensor")
    rows = part.shape[0]
    chunk = 32 if rows % 32 == 0 else rows
    dma = pltpu.SemaphoreType.DMA
    vmem = pl.BlockSpec(memory_space=pltpu.VMEM)
    return pl.pallas_call(
        functools.partial(hidden_kernel, members, chunk),
        out_shape=jax.ShapeDtypeStruct(part.shape, part.dtype),
        in_specs=[vmem],
        out_specs=vmem,
        scratch_shapes=[
            pltpu.VMEM((members,) + part.shape, part.dtype),
            dma((members * (rows // chunk),)),
            dma((members * (rows // chunk),)),
        ],
        compiler_params=pltpu.CompilerParams(collective_id=2, has_side_effects=True),
    )(part)


def expert_rows(tok_rows, w_in, w_out):
    partial_sum = jnp.einsum("rd,df->rf", tok_rows, w_in, preferred_element_type=jnp.float32)
    hidden = hidden_rows(partial_sum.astype(jnp.bfloat16))
    return jnp.einsum("rf,fd->rd", hidden, w_out, preferred_element_type=jnp.float32)


def slots_of(rows):
    return -(-rows // 128) * 128


def layer_kernel(dims, residual, queries, keys, values, lengths, gain, names, shares, w_in, w_out,
                 out, win, wout, summed, heads, named, slot_square, square_in, gath, tiles, nrm, tok, pick, pick_t, slot_weight, sendx, gotx, acc, part, part_in, hidden,
                 sendy, goty, weighted, line_out, line_in, direct_in, fin, extra,
                 kv_sem, in_sem, out_sem, sq_sem, gath_sem, tile_sem, first_sem, line_sem, third_sem, part_sem,
                 back_sem, relay_sem, direct_sem, home_sem):
    lines, planes, owners, chunks, capacity = dims
    tokens, width = residual.shape
    members = planes * owners
    places = lines * members
    quarter = width // members
    cols = quarter // chunks
    group = members * tokens
    slots = slots_of(capacity)
    units = w_in.shape[1]
    me = lax.axis_index("dp")
    line, spot = lax.div(me, members), lax.rem(me, members)
    own_plane = lax.div(spot, owners)
    other_core = 1 - lax.axis_index("tensor")
    f32, bf16 = jnp.float32, jnp.bfloat16

    def far(source, target, send, recv, device):
        return pltpu.make_async_remote_copy(
            src_ref=source, dst_ref=target, send_sem=send, recv_sem=recv, device_id=device,
            device_id_type=MESH,
        )

    def arrived(shape_like, recv):
        far(shape_like, shape_like, recv, recv, {"tensor": other_core}).wait_recv()

    def departed(shape_like, send):
        far(shape_like, shape_like, send, send, {"tensor": other_core}).wait_send()

    def peer(step):
        return lax.rem(spot + step, members)

    def sender(step):
        return lax.rem(spot + members - step, members)

    def place(index):
        return {"dp": line * members + index}

    def along(gap):
        return {"dp": lax.rem(line + gap, lines) * members + spot}

    steps = range(1, members)
    last = members - 1
    depth = members * cols
    width_kv = keys.shape[1]
    cache = keys.shape[0] // tokens
    per_kv = width_kv // HEAD
    per_group = HEADS // KV
    count = width // HEAD
    batches = kv_sem.shape[0]
    batch = tokens // batches

    def kv_copies(i):
        rows = pl.ds(i * batch * cache, batch * cache)
        return [
            pltpu.make_async_copy(keys.at[rows], wout.at[rows, pl.ds(0, width_kv)], kv_sem.at[i]),
            pltpu.make_async_copy(
                values.at[rows], wout.at[rows, pl.ds(width_kv, width_kv)], kv_sem.at[i]
            ),
        ]

    def win_copy(i):
        c, q = lax.div(i, members), lax.rem(i, members)
        return pltpu.make_async_copy(
            w_in.at[pl.ds(pl.multiple_of(q * quarter + c * cols, cols), cols)],
            win.at[pl.ds(pl.multiple_of(i * cols, cols), cols)],
            in_sem.at[c],
        )

    pieces = 8
    piece = units // pieces
    wout_copies = [
        pltpu.make_async_copy(
            w_out.at[pl.ds(i * piece, piece)], wout.at[pl.ds(i * piece, piece)], out_sem.at[0]
        )
        for i in range(pieces)
    ]
    barrier = pltpu.get_barrier_semaphore()
    for step in steps:
        pl.semaphore_signal(barrier, inc=1, device_id=place(peer(step)), device_id_type=MESH)
    for gap in range(1, lines):
        pl.semaphore_signal(barrier, inc=1, device_id=along(gap), device_id_type=MESH)
    pl.semaphore_signal(barrier, inc=1, device_id={"tensor": other_core}, device_id_type=MESH)
    for i in range(batches):
        for copy in kv_copies(i):
            copy.start()
    for h in range(count):
        heads[pl.ds(h, tokens, stride=count)] = queries[:, h * HEAD:(h + 1) * HEAD].astype(f32)
    head_row = lax.broadcasted_iota(jnp.int32, (count, HEAD), 0)
    owned = [
        (head_row >= g * per_group) & (head_row < (g + 1) * per_group) for g in range(per_kv)
    ]
    position = lax.broadcasted_iota(jnp.int32, (count, cache), 1)
    feeds = -(-members * chunks // batches)

    @pl.loop(0, batches)
    def _(i):
        rows = pl.ds(i * batch * cache, batch * cache)
        whole = wout.at[rows, pl.ds(0, 2 * width_kv)]
        pltpu.make_async_copy(w_out.at[pl.ds(0, batch * cache), pl.ds(0, 2 * width_kv)], whole,
                              kv_sem.at[i]).wait()
        for k in range(feeds):
            @pl.when(i * feeds + k < members * chunks)
            def _():
                win_copy(i * feeds + k).start()
        probs = []
        for j in range(batch):
            t = i * batch + j
            query = heads[pl.ds(pl.multiple_of(t * count, 8), count)]
            query = jnp.concatenate(
                [jnp.where(mask, query, 0.0) for mask in owned], axis=1
            ).astype(bf16)
            key = wout[pl.ds(pl.multiple_of(t * cache, cache), cache), 0:width_kv]
            score = lax.dot_general(query, key, (((1,), (1,)), ((), ())),
                                    preferred_element_type=f32) * HEAD ** (-0.5)
            score = jnp.where(position < lengths[t], score, -1e30)
            powered = jnp.exp(score - jnp.max(score, axis=1, keepdims=True))
            probs.append(
                (powered / jnp.sum(powered, axis=1, keepdims=True)).astype(bf16)
            )
        for j in range(batch):
            t = i * batch + j
            value = wout[pl.ds(pl.multiple_of(t * cache, cache), cache), width_kv:2 * width_kv]
            mixed = jnp.dot(probs[j], value, preferred_element_type=f32)
            attended = jnp.where(owned[0], mixed[:, 0:HEAD], 0.0)
            for g in range(1, per_kv):
                attended += jnp.where(owned[g], mixed[:, g * HEAD:(g + 1) * HEAD], 0.0)
            heads[pl.ds(pl.multiple_of(t * count, 8), count)] = attended

    for copy in wout_copies:
        copy.start()
    total = jnp.zeros((tokens, 1), f32)
    for h in range(count):
        at = h * HEAD
        value = residual[:, at:at + HEAD].astype(f32) + heads[pl.ds(h, tokens, stride=count)]
        summed[:, at:at + HEAD] = value
        total += jnp.sum(value * value, axis=1, keepdims=True)
    square_row = jnp.broadcast_to(total, (tokens, 128)).T[0:1]
    lane = lax.broadcasted_iota(jnp.int32, (8, group), 1)
    here = (lane >= spot * tokens) & (lane < spot * tokens + tokens)
    labels = jnp.concatenate(
        [names[...].astype(f32), shares[...], square_row, jnp.zeros((3, tokens), f32)], axis=0
    )
    named[...] = jnp.where(here, jnp.concatenate([labels] * members, axis=1), 0.0)
    pl.semaphore_wait(barrier, members + lines - 1)
    for step in steps:
        far(named, gath.at[spot], gath_sem.at[0], gath_sem.at[1], place(peer(step))).start()
    gath[spot] = named[...]
    for c in range(chunks):
        for q in range(members):
            at = q * quarter + c * cols
            nrm[q, c] = (
                summed[:, at:at + cols] * gain[at:at + cols].astype(f32)[None, :]
            ).astype(bf16)
        home = pl.ds(pl.multiple_of(line * group + spot * tokens, tokens), tokens)
        tok[c, home] = nrm[spot, c]
        for step in steps:
            far(nrm.at[peer(step), c], tok.at[c, home], first_sem.at[chunks], first_sem.at[c],
                place(peer(step))).start()

    arrived(gath.at[pl.ds(0, last)], gath_sem.at[1])
    tile = gath[0]
    for m in range(1, members):
        tile += gath[m]
    tiles[line] = tile
    for gap in range(1, lines):
        far(tiles.at[line], tiles.at[line], tile_sem.at[0], tile_sem.at[1], along(gap)).start()

    def rows_of(plane):
        return pl.ds(pl.multiple_of(plane * group, group), group)

    def inside(plane):
        return (plane >= 0) & (plane < lines)

    def spread(way, c, gap):
        turn = 1 - 2 * way
        plane = line - gap * turn
        rows = rows_of(plane)
        return inside(plane) & inside(line + turn), far(
            tok.at[c, rows], tok.at[c, rows], line_sem.at[2 * chunks * lines + way],
            line_sem.at[(way * chunks + c) * lines + plane], {"dp": me + turn * members},
        )

    def arrive(way, c, gap):
        plane = line - gap * (1 - 2 * way)

        @pl.when(inside(plane))
        def _():
            arrived(tok.at[c, rows_of(plane)], line_sem.at[(way * chunks + c) * lines + plane])

    def begin(pair):
        @pl.when(pair[0])
        def _():
            pair[1].start()

    for c in range(chunks):
        arrived(nrm.at[pl.ds(0, last), c], first_sem.at[c])
        for way in (0, 1):
            begin(spread(way, c, 0))

    arrived(tiles.at[pl.ds(0, lines - 1)], tile_sem.at[1])
    hits, weights, tile_squares = [], [], []
    for p in range(lines):
        tile = tiles[p]
        tile_squares.append(tile[4:5])
        for b in range(planes):
            expert = (line * planes + b).astype(f32)
            first, second = tile[0:1] == expert, tile[1:2] == expert
            hits.append(jnp.where(first | second, 1.0, 0.0))
            weights.append(jnp.where(first, tile[2:3], jnp.where(second, tile[3:4], 0.0)))
    earlier = lax.broadcasted_iota(jnp.int32, (group, group), 0)
    later = lax.broadcasted_iota(jnp.int32, (group, group), 1)
    before = jnp.where(earlier < later, 1.0, 0.0).astype(bf16)
    slot_iota = lax.broadcasted_iota(jnp.int32, (slots, group), 0).astype(f32)
    for b in range(planes):
        offset = jnp.zeros((1, 1), f32)
        slot_total = jnp.zeros((slots, 1), f32)
        square_total = jnp.zeros((slots, 1), f32)
        for p in range(lines):
            hit, weight = hits[p * planes + b], weights[p * planes + b]
            wide = jnp.broadcast_to(hit, (16, group)).astype(bf16)
            rank = jnp.dot(wide, before, preferred_element_type=f32)[0:1] + offset
            offset += jnp.sum(hit, axis=1, keepdims=True)
            rank = jnp.where((hit > 0.0) & (rank < capacity), rank, -1.0)
            chosen = jnp.where(slot_iota == rank, 1.0, 0.0)
            pick[b * slots:(b + 1) * slots, p * group:(p + 1) * group] = chosen.astype(bf16)
            pick_t[p, :, b * slots:(b + 1) * slots] = chosen.T.astype(bf16)
            slot_total += jnp.sum(chosen * weight, axis=1, keepdims=True)
            square_total += jnp.sum(chosen * tile_squares[p], axis=1, keepdims=True)
        slot_weight[b * slots:(b + 1) * slots] = jnp.broadcast_to(slot_total, (slots, 128))
        slot_square[b * slots:(b + 1) * slots] = jnp.broadcast_to(square_total, (slots, 128))
    own_slots = pl.multiple_of(own_plane * slots, slots)
    far(slot_square.at[pl.ds(own_slots, slots)], square_in, sq_sem.at[0], sq_sem.at[1],
        {"tensor": other_core}).start()
    weighted[...] = jnp.zeros_like(weighted)

    def lanes_of(index):
        return pl.ds(pl.multiple_of(index * cols, 128), cols)

    spans = part.shape[0]
    span = units // spans
    block = 512
    slab = 256

    def product(c, at):
        return jnp.dot(gotx[c], win[c * depth:(c + 1) * depth, at], preferred_element_type=f32)

    def expand(c):
        arrived(goty.at[c, pl.ds(0, last)], third_sem.at[c])
        pltpu.make_async_copy(w_in.at[pl.ds(0, depth)], win.at[pl.ds(c * depth, depth)],
                              in_sem.at[c]).wait()
        @pl.loop(0, spans)
        def _(h):
            for inner in range(0, span, slab):
                at = pl.ds(pl.multiple_of(h * span + inner, slab), slab)
                value = product(c, at)
                if c:
                    value += acc[:, at]
                if c < chunks - 1:
                    acc[:, at] = value
                else:
                    part[h, :, inner:inner + slab] = value.astype(bf16)
            if c == chunks - 1:
                far(part.at[h], part_in.at[h], part_sem.at[spans], part_sem.at[h],
                    {"tensor": other_core}).start()

    for c in range(chunks):
        for gap in range(1, lines):
            for way in (0, 1):
                arrive(way, c, gap)
                begin(spread(way, c, gap))
        rows = jnp.dot(pick[...], tok[c], preferred_element_type=f32).astype(bf16)
        for b in range(planes):
            sendx[c, b] = rows[b * slots:b * slots + capacity]
        for step in steps:
            far(sendx.at[c, lax.div(peer(step), owners)], gotx.at[c, :, lanes_of(spot)],
                third_sem.at[chunks], third_sem.at[c], place(peer(step))).start()
        gotx[c, :, lanes_of(spot)] = sendx[c, own_plane]
        if c:
            expand(c - 1)
    expand(chunks - 1)
    arrived(square_in, sq_sem.at[1])
    scale = lax.rsqrt(
        (slot_square[pl.ds(own_slots, capacity), :1] + square_in[0:capacity, :1]) / (2 * width)
        + NORM_EPSILON
    )
    for h in range(spans):
        arrived(part_in.at[h], part_sem.at[h])

        @pl.loop(0, span // block)
        def _(i):
            at = pl.ds(pl.multiple_of(i * block, block), block)
            value = (part[h, :, at].astype(f32) + part_in[h, :, at].astype(f32)) * scale
            value = value / (1.0 + jnp.exp(-value))
            hidden[:, pl.ds(pl.multiple_of(h * span + i * block, block), block)] = (
                value.astype(bf16)
            )
    pltpu.make_async_copy(w_out, wout, out_sem.at[0]).wait()

    joined = 1

    def contract(c):
        for step in list(steps) + [0]:
            at = pl.multiple_of(peer(step) * quarter + c * cols, 128)
            value = jnp.dot(hidden[...], wout[:, pl.ds(at, joined * cols)],
                            preferred_element_type=f32).astype(bf16)
            for k in range(joined):
                inner = value[:, k * cols:(k + 1) * cols]
                if step:
                    sendy[c + k, step - 1] = inner
                    far(sendy.at[c + k, step - 1], goty.at[c + k, spot], back_sem.at[chunks],
                        back_sem.at[c + k], place(peer(step))).start()
                else:
                    goty[c + k, spot] = inner

    def gather_back(c):
        arrived(sendy.at[c], back_sem.at[c])
        for b in range(planes):
            value = goty[c, b * owners].astype(f32)
            for o in range(1, owners):
                value += goty[c, b * owners + o].astype(f32)
            value = value * slot_weight[b * slots:b * slots + capacity, :1]
            weighted[c, b * slots:b * slots + capacity] = value.astype(bf16)

    def share(c, plane):
        return jnp.dot(pick_t[plane], weighted[c], preferred_element_type=f32)

    def relay_mark(way, c, plane):
        return relay_sem.at[(way * chunks + c) * lines + plane]

    def relay(way, c, gap):
        turn = 1 - 2 * way
        plane = line + gap * turn

        @pl.when(inside(plane))
        def _():
            value = share(c, plane)
            line_out[way, c, plane] = value.astype(bf16)

            if gap == lines - 1:
                far(line_out.at[way, c, plane], direct_in.at[c], direct_sem.at[chunks],
                    direct_sem.at[c], {"dp": me + turn * gap * members}).start()
                return
            if gap + 1 < lines - 1:
                @pl.when(inside(line - turn))
                def _():
                    arrived(line_in.at[way, c, plane], relay_mark(way, c, plane))
                    line_out[way, c, plane] = (
                        value + line_in[way, c, plane].astype(f32)
                    ).astype(bf16)

            far(line_out.at[way, c, plane], line_in.at[way, c, plane],
                relay_sem.at[2 * chunks * lines + way], relay_mark(way, c, plane),
                {"dp": me + turn * members}).start()

    near = jnp.where(line * 2 < lines, 0, 1)

    def finish(c):
        for way in (0, 1):
            turn = 1 - 2 * way

            @pl.when(inside(line - turn))
            def _():
                arrived(line_in.at[way, c, line], relay_mark(way, c, line))

        low, high = line > 0, line < lines - 1

        def got(way):
            return line_in[way, c, line].astype(f32)

        @pl.when(low & high)
        def _():
            fin[c] = (share(c, line) + got(0) + got(1)).astype(bf16)

        @pl.when(low & ~high)
        def _():
            arrived(direct_in.at[c], direct_sem.at[c])
            fin[c] = (share(c, line) + got(0) + direct_in[c].astype(f32)).astype(bf16)

        @pl.when(high & ~low)
        def _():
            arrived(direct_in.at[c], direct_sem.at[c])
            fin[c] = (share(c, line) + got(1) + direct_in[c].astype(f32)).astype(bf16)

        for step in steps:
            rows = pl.ds(pl.multiple_of(peer(step) * tokens, tokens), tokens)
            far(fin.at[c, rows], extra.at[c, spot], home_sem.at[chunks], home_sem.at[c],
                place(peer(step))).start()
        extra[c, spot] = fin[c, pl.ds(pl.multiple_of(spot * tokens, tokens), tokens)]

    def close(c):
        arrived(extra.at[c, pl.ds(0, last)], home_sem.at[c])
        for q in range(members):
            at = q * quarter + c * cols
            out[:, at:at + cols] = (
                summed[:, at:at + cols] + extra[c, q].astype(f32)
            ).astype(out.dtype)

    for c in range(0, chunks, joined):
        contract(c)
    for c in range(chunks):
        gather_back(c)
        for gap in list(range(lines - 2, 1, -1)) + [lines - 1]:
            relay(near, c, gap)
    for c in range(chunks):
        relay(near, c, 1)
    for c in range(chunks):
        for gap in range(lines - 2, 0, -1):
            relay(1 - near, c, gap)
    for c in range(chunks):
        finish(c)
        if c:
            close(c - 1)
    close(chunks - 1)
    departed(square_in, sq_sem.at[0])
    departed(gath.at[pl.ds(0, last)], gath_sem.at[0])
    departed(tiles.at[pl.ds(0, lines - 1)], tile_sem.at[0])
    departed(nrm.at[pl.ds(0, last)], first_sem.at[chunks])
    departed(goty.at[:, pl.ds(0, last)], third_sem.at[chunks])
    departed(part, part_sem.at[spans])
    departed(sendy, back_sem.at[chunks])
    departed(extra.at[:, pl.ds(0, last)], home_sem.at[chunks])
    base = 2 * chunks * lines
    for at in range(lines):
        @pl.when(line == at)
        def _():
            above, below = lines - 1 - at, at
            if above:
                departed(tok.at[:, pl.ds(0, (below + 1) * group)], line_sem.at[base])
                sent = above if below else above - 1
                departed(line_out.at[0, :, pl.ds(0, sent)], relay_sem.at[base])
            if below:
                departed(tok.at[:, pl.ds(0, (above + 1) * group)], line_sem.at[base + 1])
                sent = below if above else below - 1
                departed(line_out.at[1, :, pl.ds(0, sent)], relay_sem.at[base + 1])
            if not above or not below:
                departed(direct_in, direct_sem.at[chunks])


def layer(residual, queries, keys, values, lengths, gain, names, shares, w_in, w_out, lines,
          planes, owners, capacity, chunks):
    tokens, width = residual.shape
    members = planes * owners
    cols = width // members // chunks
    places = lines * members
    group = members * tokens
    slots = slots_of(capacity)
    units = w_in.shape[1]
    spans, batches = 4, 4
    f32, bf16 = jnp.float32, jnp.bfloat16
    vmem = pl.BlockSpec(memory_space=pltpu.VMEM)
    hbm = pl.BlockSpec(memory_space=pl.ANY)
    dma = pltpu.SemaphoreType.DMA
    return pl.pallas_call(
        functools.partial(layer_kernel, (lines, planes, owners, chunks, capacity)),
        out_shape=jax.ShapeDtypeStruct((tokens, width), bf16),
        in_specs=[vmem, vmem, hbm, hbm, pl.BlockSpec(memory_space=pltpu.SMEM), vmem, vmem, vmem,
                  hbm, hbm],
        out_specs=vmem,
        scratch_shapes=[
            pltpu.VMEM(w_in.shape, bf16),
            pltpu.VMEM(w_out.shape, bf16),
            pltpu.VMEM((tokens, width), f32),
            pltpu.VMEM((tokens * width // HEAD, HEAD), f32),
            pltpu.VMEM((8, group), f32),
            pltpu.VMEM((planes * slots, 128), f32),
            pltpu.VMEM((slots, 128), f32),
            pltpu.VMEM((members, 8, group), f32),
            pltpu.VMEM((lines, 8, group), f32),
            pltpu.VMEM((members, chunks, tokens, cols), bf16),
            pltpu.VMEM((chunks, lines * group, cols), bf16),
            pltpu.VMEM((planes * slots, lines * group), bf16),
            pltpu.VMEM((lines, group, planes * slots), bf16),
            pltpu.VMEM((planes * slots, 128), f32),
            pltpu.VMEM((chunks, planes, capacity, cols), bf16),
            pltpu.VMEM((chunks, capacity, members * cols), bf16),
            pltpu.VMEM((capacity, units), f32),
            pltpu.VMEM((spans, capacity, units // spans), bf16),
            pltpu.VMEM((spans, capacity, units // spans), bf16),
            pltpu.VMEM((capacity, units), bf16),
            pltpu.VMEM((chunks, members - 1, capacity, cols), bf16),
            pltpu.VMEM((chunks, members, capacity, cols), bf16),
            pltpu.VMEM((chunks, planes * slots, cols), bf16),
            pltpu.VMEM((2, chunks, lines, group, cols), bf16),
            pltpu.VMEM((2, chunks, lines, group, cols), bf16),
            pltpu.VMEM((chunks, group, cols), bf16),
            pltpu.VMEM((chunks, group, cols), bf16),
            pltpu.VMEM((chunks, members, tokens, cols), bf16),
            dma((batches,)),
            dma((chunks,)),
            dma((1,)),
            dma((2,)),
            dma((2,)),
            dma((2,)),
            dma((chunks + 1,)),
            dma((2 * chunks * lines + 2,)),
            dma((chunks + 1,)),
            dma((spans + 1,)),
            dma((chunks + 1,)),
            dma((2 * chunks * lines + 2,)),
            dma((chunks + 1,)),
            dma((chunks + 1,)),
        ],
        compiler_params=pltpu.CompilerParams(
            collective_id=3, has_side_effects=True, vmem_limit_bytes=63 * 1024 * 1024
        ),
    )(residual, queries, keys, values, lengths, gain, names, shares, w_in, w_out)


def planes_of(places, tokens, width, width_kv, units, capacity):
    owners, rest = divmod(places, EXPERTS)
    planes = 2
    members = planes * owners
    if rest or lax.axis_size("tensor") != 2 or members < 2 or members * tokens != 128:
        return 0
    if EXPERTS // planes < 3 or width % (members * 128) or units % 2048 or capacity % 16:
        return 0
    if tokens * CACHE > units or 2 * width_kv > width or CACHE % 128 or HEAD != 128:
        return 0
    held = 4 * units * width + 12 * capacity * units
    return planes if held < 56 * 1024 * 1024 else 0


def shards(
    residual, queries, keys, values, lengths, norm_gain, expert_ids, expert_weights, w_in, w_out
):
    tokens = residual.shape[0]
    width_local = residual.shape[1]
    places = lax.axis_size("dp")
    capacity = tokens * places * TOPK * 3 // (4 * EXPERTS)
    width_kv = keys.shape[2]
    planes = planes_of(places, tokens, width_local, width_kv, w_in.shape[1], capacity)
    if planes:
        return layer(
            residual, queries, keys.reshape(-1, width_kv), values.reshape(-1, width_kv), lengths,
            norm_gain, expert_ids.T, expert_weights.T, w_in, w_out, EXPERTS // planes,
            planes, places // EXPERTS, capacity, 2,
        )
    head_groups = keys.shape[2] // HEAD
    group_size = HEADS // KV
    query_rows = queries.reshape(tokens, head_groups, group_size, HEAD)
    key_rows = keys.reshape(tokens, CACHE, head_groups, HEAD)
    value_rows = values.reshape(tokens, CACHE, head_groups, HEAD)
    scores = jnp.einsum(
        "tgjd,tlgd->tgjl", query_rows, key_rows, preferred_element_type=jnp.float32
    ) * HEAD ** (-0.5)
    live_mask = (jnp.arange(CACHE, dtype=jnp.int32)[None, :] < lengths[:, None])[:, None, None, :]
    scores = jnp.where(live_mask, scores, -1e30)
    peak_score = jnp.max(scores, axis=-1, keepdims=True)
    powered = jnp.exp(scores - peak_score)
    attention_probs = (powered / jnp.sum(powered, axis=-1, keepdims=True)).astype(jnp.bfloat16)
    attended = jnp.einsum(
        "tgjl,tlgd->tgjd", attention_probs, value_rows, preferred_element_type=jnp.float32
    )
    summed = residual.astype(jnp.float32) + attended.reshape(tokens, width_local)
    square_sums = lax.psum(jnp.sum(summed * summed, axis=1), "tensor")
    normed = (
        summed
        * lax.rsqrt(square_sums[:, None] / D + NORM_EPSILON)
        * norm_gain.astype(jnp.float32)[None, :]
    ).astype(jnp.bfloat16)
    flat_ids = expert_ids.reshape(-1)
    expert_iota = jnp.arange(EXPERTS, dtype=jnp.int32)
    onehot = (flat_ids[:, None] == expert_iota[None, :]).astype(jnp.int32)
    local_rank = jnp.sum(
        (jnp.cumsum(onehot, axis=0, dtype=jnp.int32) - onehot) * onehot, axis=1, dtype=jnp.int32
    )
    counts = jnp.sum(onehot, axis=0, dtype=jnp.int32)
    me = lax.axis_index("dp")
    owners = places // EXPERTS
    slot_total = EXPERTS * SRC_CAP
    pair_target = flat_ids * SRC_CAP + local_rank
    pick_pairs = pair_target[None, :] == jnp.arange(slot_total, dtype=jnp.int32)[:, None]
    pick_tokens = jnp.sum(
        pick_pairs.reshape(slot_total, tokens, TOPK).astype(jnp.float32), axis=2
    ).astype(jnp.bfloat16)
    packed = jnp.dot(pick_tokens, normed, preferred_element_type=jnp.float32).astype(jnp.bfloat16)
    padded_counts = jnp.pad(counts[None, :], ((0, 0), (0, 128 - EXPERTS)))
    received, gathered = dispatch(
        packed.reshape(EXPERTS, SRC_CAP, width_local), padded_counts, owners
    )
    all_counts = gathered[:, 0, :EXPERTS]
    place_iota = jnp.arange(places, dtype=jnp.int32)
    offsets = jnp.sum(jnp.where(place_iota[:, None] < me, all_counts, 0), axis=0, dtype=jnp.int32)
    slot_index = local_rank + jnp.sum(onehot * offsets[None, :], axis=1, dtype=jnp.int32)
    keep_mask = slot_index < capacity
    mine = jnp.sum(
        jnp.where(expert_iota[None, :] == me // owners, all_counts, 0), axis=1, dtype=jnp.int32
    )
    before = jnp.sum(
        jnp.where(place_iota[None, :] < place_iota[:, None], mine[None, :], 0),
        axis=1,
        dtype=jnp.int32,
    )
    rank = jnp.arange(SRC_CAP, dtype=jnp.int32)[None, :]
    row_slot = jnp.where(rank < mine[:, None], before[:, None] + rank, -1).reshape(-1)
    pick_rows = (
        row_slot[None, :] == jnp.arange(capacity, dtype=jnp.int32)[:, None]
    ).astype(jnp.bfloat16)
    total_rows = places * SRC_CAP
    compact = jnp.dot(
        pick_rows, received.reshape(total_rows, width_local), preferred_element_type=jnp.float32
    ).astype(jnp.bfloat16)
    results = expert_rows(compact, w_in, w_out).astype(jnp.bfloat16)
    spread = jnp.einsum(
        "cr,cd->rd", pick_rows, results, preferred_element_type=jnp.float32
    ).astype(jnp.bfloat16)
    per_expert = (
        send_back(spread.reshape(places, SRC_CAP, width_local), owners)
        .reshape(slot_total, width_local)
        .astype(jnp.float32)
    )
    pair_weight = expert_weights.reshape(-1) * keep_mask.astype(jnp.float32)
    mix_rows = jnp.sum(
        (pick_pairs.astype(jnp.float32) * pair_weight[None, :]).reshape(slot_total, tokens, TOPK),
        axis=2,
    )
    addition = jnp.einsum("st,sd->td", mix_rows, per_expert, precision=lax.Precision.HIGHEST)
    return (summed + addition).astype(jnp.bfloat16)


def solution(mesh):
    in_specs = (
        P("dp", "tensor"),
        P("dp", "tensor"),
        P("dp", None, "tensor"),
        P("dp", None, "tensor"),
        P("dp"),
        P("tensor"),
        P("dp", None),
        P("dp", None),
        P("tensor", "dp"),
        P("dp", "tensor"),
    )
    out_specs = P("dp", "tensor")
    return jax.shard_map(shards, mesh=mesh, in_specs=in_specs, out_specs=out_specs, check_vma=False)
```
